256 devices in a mesh: blk: 64 (over x_hi, y, z), chan: 4 (over x_lo, core).
Axes of the slice: x: 4 (x_hi: 2, x_lo: 2; x = x_hi * 2 + x_lo), y: 4, z: 8, core: 2. Of those that a mesh axis runs over, the one named last changes fastest.
Arguments:
- pair_map: int32 [128, 2], P('blk'), may hold values from 0 to 15, as said below
- visibilities: bfloat16 [2, 128, 64, 1024], P(None, 'blk', 'chan'), may hold values from -24 to 24
- model_vis: bfloat16 [2, 128, 64, 1024], P(None, 'blk', 'chan'), may hold values from -7.2 to 7.2
- flag_mask: int32 [128, 64, 1024], P('blk', 'chan'), may hold values 0 or 1
- gain_amp: float32 [512], replicated, may hold values from 0.19 to 3.17
- gain_phase: float32 [512], replicated, may hold values from -3.1416 to 3.1416
- row_index: int32 [4, 64, 64, 256], P('chan', 'blk'), may hold values from -1 to 32767, as said below
- cell_codes: int32 [2, 4, 64, 64, 256], P(None, 'chan', 'blk'), may hold values from 32 to 992
Outputs:
- grid_tiles: float32 [4, 64, 2, 128, 128], P('chan', 'blk')
- solved_gains: float32 [2, 512], replicated
The draws below stay inside these ranges and needn't reach their ends.
Inputs may be any that keep to these rules, and one draw needn't show every extreme that they name: `pair_map`: each row is a pair (p, q) of station blocks with p <= q; no two rows are the same pair; every station block appears in some row. `row_index`: each visibility of an index of blk and a channel group appears in at most one row of that index and group; about half of the rows are -1.
All inputs are finite; a program needn't handle non-finite values. No bound on the sum of `flag_mask` on one device may be relied on, other than what follows from the above.
Results may differ from the reference program's by a relative error of at most 0.009.
Values may be sent and summed in bfloat16 or wider, within the bound.
A program may use at most 64 MiB of HBM per device.

```python
import math
import jax
import jax.numpy as jnp
import numpy as np
from jax import lax

S = 512
BS = 32
PAIRS_DEV = 2
SENDERS = 64
PAIRS = 128
CH_DEV = 16
GROUPS = 4
CHANNELS = 64
ITERS = 3
TS = 128
TILES = 64
CAP = 2
KS = 8
OVER = 8


def pair_table(key):
    block_count = S // BS
    first_np, second_np = np.triu_indices(block_count)
    pair_count = first_np.shape[0]
    shuffled = jax.random.permutation(jax.random.fold_in(key, 101), block_count).astype(jnp.int32)
    half = block_count // 2
    lower_block = jnp.minimum(shuffled[0:2 * half:2], shuffled[1:2 * half:2])
    upper_block = jnp.maximum(shuffled[0:2 * half:2], shuffled[1:2 * half:2])
    covered = lower_block * block_count - lower_block * (lower_block - 1) // 2 + (upper_block - lower_block)
    scores = jax.random.randint(jax.random.fold_in(key, 102), (pair_count,), 0, 1 << 20, dtype=jnp.int32) * 1024
    scores = scores + jnp.arange(pair_count, dtype=jnp.int32)
    scores = scores.at[covered].set(-1 - jnp.arange(half, dtype=jnp.int32))
    chosen = jnp.argsort(scores, stable=True)[:PAIRS]
    first_col = jnp.asarray(first_np, dtype=jnp.int32)[chosen]
    second_col = jnp.asarray(second_np, dtype=jnp.int32)[chosen]
    return jnp.stack((first_col, second_col), axis=1)


def model_values(key):
    full_shape = (2, PAIRS, CHANNELS, BS * BS)
    pattern = jnp.clip(jax.random.normal(jax.random.fold_in(key, 201), full_shape, jnp.float32), -4.0, 4.0)
    spectral = 0.6 + 1.2 * jnp.arange(CHANNELS, dtype=jnp.float32) / max(CHANNELS - 1, 1)
    return pattern * spectral[None, None, :, None]


def station_truth(key):
    amplitude = jax.random.uniform(jax.random.fold_in(key, 301), (S,), jnp.float32, 0.6, 1.4)
    phases = jax.random.uniform(jax.random.fold_in(key, 302), (S,), jnp.float32, -math.pi, math.pi)
    return (amplitude, phases)


def draw_pair_map(key, part):
    return pair_table(key)


def draw_model_vis(key, part):
    return model_values(key).astype(jnp.bfloat16)


def draw_gain_amp(key, part):
    amplitude, phases = station_truth(key)
    lower_scale = jax.random.uniform(jax.random.fold_in(key, 501), (), jnp.float32, 0.55, 0.7)
    upper_scale = jax.random.uniform(jax.random.fold_in(key, 502), (), jnp.float32, 1.4, 1.8)
    picked = jax.random.randint(jax.random.fold_in(key, 503), (), 0, 2, dtype=jnp.int32)
    common = jnp.where(picked == 1, upper_scale, lower_scale)
    jitter = jax.random.uniform(jax.random.fold_in(key, 504), (S,), jnp.float32, 0.9, 1.1)
    return (amplitude * common * jitter).astype(jnp.float32)


def draw_gain_phase(key, part):
    amplitude, phases = station_truth(key)
    common = jax.random.uniform(jax.random.fold_in(key, 505), (), jnp.float32, -math.pi, math.pi)
    jitter = jax.random.uniform(jax.random.fold_in(key, 506), (S,), jnp.float32, -0.3, 0.3)
    angle_sum = phases + common + jitter
    return jnp.arctan2(jnp.sin(angle_sum), jnp.cos(angle_sum)).astype(jnp.float32)


def draw_visibilities(key, part):
    model_full = model_values(key)
    pairs = pair_table(key)
    baseline = jnp.arange(BS * BS, dtype=jnp.int32)
    first_station = pairs[:, 0:1] * BS + baseline[None, :] // BS
    second_station = pairs[:, 1:2] * BS + baseline[None, :] % BS
    amplitude, phases = station_truth(key)
    noise_level = 0.3
    true_real = amplitude * jnp.cos(phases)
    true_imag = amplitude * jnp.sin(phases)
    first_real = true_real[first_station][:, None, :]
    first_imag = true_imag[first_station][:, None, :]
    second_real = true_real[second_station][:, None, :]
    second_imag = true_imag[second_station][:, None, :]
    twisted_real = model_full[0] * second_real + model_full[1] * second_imag
    twisted_imag = model_full[1] * second_real - model_full[0] * second_imag
    noise_terms = jnp.clip(jax.random.normal(jax.random.fold_in(key, 303), model_full.shape, jnp.float32), -4.0, 4.0)
    vis_real = first_real * twisted_real - first_imag * twisted_imag + noise_level * noise_terms[0]
    vis_imag = first_real * twisted_imag + first_imag * twisted_real + noise_level * noise_terms[1]
    return jnp.stack((vis_real, vis_imag)).astype(jnp.bfloat16)


def draw_row_index(key, part):
    visible = PAIRS_DEV * CH_DEV * BS * BS
    row_total = TILES * CAP * 128
    device_keys = jax.random.split(jax.random.fold_in(key, 401), GROUPS * SENDERS)

    def one_device(device_key):
        shuffled = jax.random.permutation(device_key, 2 * visible).astype(jnp.int32)[:row_total]
        return jnp.where(shuffled < visible, shuffled, -1).astype(jnp.int32)
    picked = jax.vmap(one_device)(device_keys)
    return picked.reshape(GROUPS, SENDERS, TILES, CAP * 128)


def touch_ends(result, stream_key, smallest, largest):
    longest = result.shape.index(max(result.shape))
    spots = []
    for shift in (0, 1):
        where = [jax.random.randint(jax.random.fold_in(stream_key, axis), (), 0, length) for axis, length in enumerate(result.shape)]
        where[longest] = (where[longest] + shift) % result.shape[longest]
        spots.append(tuple(where))
    return result.at[spots[0]].set(smallest).at[spots[1]].set(largest)


def setup_inputs(seed: int = 0) -> dict:
    key_of = jax.random.split(jax.random.key(seed), 9)
    return {
        "pair_map": draw_pair_map(jax.random.fold_in(key_of[8], 71), 0),
        "visibilities": draw_visibilities(jax.random.fold_in(key_of[8], 71), 0),
        "model_vis": draw_model_vis(jax.random.fold_in(key_of[8], 71), 0),
        "flag_mask": touch_ends((jax.random.randint(key_of[3], (PAIRS, CHANNELS, BS * BS), 0, 10) < 9).astype(jnp.int32), jax.random.fold_in(key_of[3], 1), 0, 1),
        "gain_amp": draw_gain_amp(jax.random.fold_in(key_of[8], 71), 0),
        "gain_phase": draw_gain_phase(jax.random.fold_in(key_of[8], 71), 0),
        "row_index": draw_row_index(jax.random.fold_in(key_of[8], 71), 0),
        "cell_codes": touch_ends(jax.random.randint(key_of[7], (2, GROUPS, SENDERS, TILES, CAP * 128), (KS // 2) * OVER, (TS - KS // 2) * OVER + 1), jax.random.fold_in(key_of[7], 1), (KS // 2) * OVER, ((TS - KS // 2) * OVER + 1) - 1).astype(jnp.int32),
    }


def kernel_rows(code_values):
    centre = code_values.astype(jnp.float32) / OVER
    cell_axis = jnp.arange(TS, dtype=jnp.float32)
    offset = cell_axis - centre[..., None]
    inside = jnp.abs(offset) < 0.5 * KS
    return jnp.where(inside, jnp.cos(math.pi * offset / KS) ** 2, 0.0).astype(jnp.bfloat16)


def reference(pair_map, visibilities, model_vis, flag_mask, gain_amp, gain_phase, row_index, cell_codes):
    baseline = jnp.arange(BS * BS, dtype=jnp.int32)
    first_station = pair_map[:, 0:1] * BS + baseline[None, :] // BS
    second_station = pair_map[:, 1:2] * BS + baseline[None, :] % BS
    weight = flag_mask.astype(jnp.float32) * (first_station != second_station).astype(jnp.float32)[:, None, :]
    vis_real = visibilities[0].astype(jnp.float32)
    vis_imag = visibilities[1].astype(jnp.float32)
    model_real = model_vis[0].astype(jnp.float32)
    model_imag = model_vis[1].astype(jnp.float32)
    cross_real = weight * (vis_real * model_real + vis_imag * model_imag)
    cross_imag = weight * (vis_imag * model_real - vis_real * model_imag)
    model_power = weight * (model_real * model_real + model_imag * model_imag)
    first_ids = jnp.broadcast_to(first_station[:, None, :], cross_real.shape).reshape(-1)
    second_ids = jnp.broadcast_to(second_station[:, None, :], cross_real.shape).reshape(-1)

    def station_sum(first_term, second_term):
        return (jax.ops.segment_sum(first_term.reshape(-1), first_ids, num_segments=S)
                + jax.ops.segment_sum(second_term.reshape(-1), second_ids, num_segments=S))

    gain_real = gain_amp * jnp.cos(gain_phase)
    gain_imag = gain_amp * jnp.sin(gain_phase)
    for sweep_index in range(ITERS):
        first_real = gain_real[first_station][:, None, :]
        first_imag = gain_imag[first_station][:, None, :]
        second_real = gain_real[second_station][:, None, :]
        second_imag = gain_imag[second_station][:, None, :]
        numerator_real = station_sum(cross_real * second_real - cross_imag * second_imag,
                                     cross_real * first_real + cross_imag * first_imag)
        numerator_imag = station_sum(cross_real * second_imag + cross_imag * second_real,
                                     cross_real * first_imag - cross_imag * first_real)
        denominator = station_sum(model_power * (second_real * second_real + second_imag * second_imag),
                                  model_power * (first_real * first_real + first_imag * first_imag))
        update_real = numerator_real / denominator
        update_imag = numerator_imag / denominator
        if sweep_index % 2 == 1:
            gain_real = 0.5 * (update_real + gain_real)
            gain_imag = 0.5 * (update_imag + gain_imag)
        else:
            gain_real = update_real
            gain_imag = update_imag

    first_real = gain_real[first_station][:, None, :]
    first_imag = gain_imag[first_station][:, None, :]
    second_real = gain_real[second_station][:, None, :]
    second_imag = gain_imag[second_station][:, None, :]
    twisted_real = model_real * second_real + model_imag * second_imag
    twisted_imag = model_imag * second_real - model_real * second_imag
    predicted_real = first_real * twisted_real - first_imag * twisted_imag
    predicted_imag = first_real * twisted_imag + first_imag * twisted_real
    resid_real = (weight * (vis_real - predicted_real)).astype(jnp.bfloat16)
    resid_imag = (weight * (vis_imag - predicted_imag)).astype(jnp.bfloat16)

    def localize(values):
        shaped = values.reshape(SENDERS, PAIRS_DEV, GROUPS, CH_DEV, BS * BS)
        return jnp.transpose(shaped, (2, 0, 1, 3, 4)).reshape(GROUPS, SENDERS, PAIRS_DEV * CH_DEV * BS * BS)

    slot_rows = row_index.reshape(GROUPS, SENDERS, TILES * CAP * 128)
    live_rows = slot_rows >= 0
    safe_rows = jnp.where(live_rows, slot_rows, 0).astype(jnp.int32)

    def pick_rows(values):
        taken = jnp.take_along_axis(localize(values), safe_rows, axis=2)
        return jnp.where(live_rows, taken, 0.0).astype(jnp.bfloat16)

    def by_tile(values):
        shaped = values.reshape(GROUPS, SENDERS, TILES, CAP * 128)
        return jnp.transpose(shaped, (0, 2, 1, 3)).reshape(GROUPS * TILES, SENDERS * CAP * 128)

    rows_real = by_tile(pick_rows(resid_real))
    rows_imag = by_tile(pick_rows(resid_imag))
    codes_u = by_tile(cell_codes[0])
    codes_v = by_tile(cell_codes[1])

    def one_tile(tile_item):
        real_rows, imag_rows, u_values, v_values = tile_item
        kernel_u = kernel_rows(u_values).astype(jnp.float32)
        kernel_v = kernel_rows(v_values).astype(jnp.float32)
        weighted = jnp.stack((kernel_v * real_rows.astype(jnp.float32)[:, None],
                              kernel_v * imag_rows.astype(jnp.float32)[:, None]), axis=1).astype(jnp.bfloat16)
        weighted = lax.optimization_barrier(weighted).astype(jnp.float32)
        return jnp.einsum("rx,rcy->cxy", kernel_u, weighted, precision=lax.Precision.HIGHEST)

    grids = lax.map(one_tile, (rows_real, rows_imag, codes_u, codes_v))
    grid_tiles = grids.reshape(GROUPS, TILES, 2, TS, TS)
    return grid_tiles, jnp.stack((gain_real, gain_imag))
```

```python
import math

import jax
import jax.numpy as jnp
from jax import lax
from jax.experimental import pallas as pl
from jax.experimental.pallas import tpu as pltpu
from jax.sharding import Mesh
from jax.sharding import PartitionSpec as P

S = 512
BS = 32
NB = 16
ITERS = 3
TS = 128
NT = 64
CH = 16
F32 = jnp.float32
BF16 = jnp.bfloat16
I32 = jnp.int32
MESH = pl.DeviceIdType.MESH
BLK = ("blk_0", "blk_1", "blk_2")
CHAN = ("chan_0", "chan_1")
VM = pl.BlockSpec(memory_space=pltpu.VMEM)
SM = pl.BlockSpec(memory_space=pltpu.SMEM)


def iota(shape, axis):
    return lax.broadcasted_iota(I32, shape, axis)


def sums_and_tables(pm_ref, vis_ref, mod_ref, flag_ref, pq_ref, table_ref):
    for slot in range(2):
        first = pm_ref[slot, 0]
        second = pm_ref[slot, 1]
        same = (first == second).astype(F32)
        lane = iota((1, 128), 1)
        planes = [[], [], [], []]
        for tb in range(8):
            at = slice(tb * 128, tb * 128 + 128)
            base = lane + tb * 128
            diagonal = ((base >> 5) == (base & 31)).astype(F32)
            weight = flag_ref[slot, :, at].astype(F32) * (1.0 - same * diagonal)
            vr = vis_ref[0, slot, :, at].astype(F32) * weight
            vi = vis_ref[1, slot, :, at].astype(F32) * weight
            mr = mod_ref[0, slot, :, at].astype(F32) * weight
            mi = mod_ref[1, slot, :, at].astype(F32) * weight
            sums = (
                jnp.sum(vr * mr + vi * mi, axis=0, keepdims=True),
                jnp.sum(vi * mr - vr * mi, axis=0, keepdims=True),
                jnp.sum(mr * mr + mi * mi, axis=0, keepdims=True),
            )
            col = slice((tb % 2) * 128, (tb % 2) * 128 + 128)
            for q in range(3):
                row = slot * 3 + q
                pq_ref[tb // 2, row : row + 1, col] = sums[q]
            for plane, value in zip(planes, (vr, vi, mr, mi)):
                plane.append(value)
        for q in range(4):
            table = jnp.concatenate(planes[q], axis=0)
            table_ref[q * 128 : q * 128 + 128, slot * 128 : slot * 128 + 128] = table.T.astype(BF16)
        for quarter in range(4):
            col = slice(slot * 128, slot * 128 + 128)
            pq_ref[quarter, 6:7, col] = jnp.full((1, 128), first.astype(F32))
            pq_ref[quarter, 7:8, col] = jnp.full((1, 128), second.astype(F32))


def gather_tile(tile, index_ref, codes_ref, table_ref, rows_ref, ints_ref):
    index = index_ref[pl.ds(tile, 1), :]
    hi = ((index >> 14) << 7) | (((index >> 7) & 7) << 4) | ((index >> 10) & 15)
    onehot = jnp.where(iota((256, 256), 0) == hi, 1.0, 0.0).astype(BF16)
    lifted = jnp.dot(table_ref[...], onehot, preferred_element_type=F32)
    low_high = (index >> 3) & 15
    low_low = index & 7
    live = iota((8, 256), 0) == low_low
    pieces = []
    masks = [jnp.broadcast_to(low_high == k, (8, 256)) for k in range(16)]
    for q in range(4):
        part = lifted[q * 128 : q * 128 + 8]
        for k in range(1, 16):
            part = jnp.where(masks[k], lifted[q * 128 + k * 8 : q * 128 + k * 8 + 8], part)
        value = jnp.sum(jnp.where(live, part, 0.0), axis=0, keepdims=True)
        pieces += [value[:, :128], value[:, 128:]]
    rows_ref[tile] = jnp.concatenate(pieces, axis=0).astype(BF16)
    u = codes_ref[0, pl.ds(tile, 1), :]
    v = codes_ref[1, pl.ds(tile, 1), :]
    both = u | (v << 16)
    place = (((index >> 14) & 1) << 10) | (index & 1023)
    ints_ref[tile] = jnp.concatenate([both[:, :128], both[:, 128:], place[:, :128], place[:, 128:]], axis=0)


def sender_kernel(pm_ref, vis_ref, mod_ref, flag_ref, index_ref, codes_ref, pq_ref, rows_ref, ints_ref, table_ref):
    sums_and_tables(pm_ref, vis_ref, mod_ref, flag_ref, pq_ref, table_ref)

    def step(tile, carry):
        gather_tile(tile, index_ref, codes_ref, table_ref, rows_ref, ints_ref)
        return carry

    lax.fori_loop(0, NT, step, 0)


def sender(pm, vis, mod, flag, index, codes):
    return pl.pallas_call(
        sender_kernel,
        name="sender",
        out_shape=(
            jax.ShapeDtypeStruct((4, 8, 256), F32),
            jax.ShapeDtypeStruct((NT, 8, 128), BF16),
            jax.ShapeDtypeStruct((NT, 4, 128), I32),
        ),
        in_specs=[SM, VM, VM, VM, VM, VM],
        out_specs=(VM, VM, VM),
        scratch_shapes=[pltpu.VMEM((512, 256), BF16)],
    )(pm, vis, mod, flag, index, codes)


def exchange_kernel(
    pq_ref, rows_ref, ints_ref, all_ref, got_rows, got_ints, part, send_sem, recv_sem, a2a_send, a2a_recv, own_sem
):
    xh, y, z = lax.axis_index("blk_0"), lax.axis_index("blk_1"), lax.axis_index("blk_2")
    xl, core = lax.axis_index("chan_0"), lax.axis_index("chan_1")
    me = (xh * 4 + y) * 8 + z
    x = xh * 2 + xl
    quarter = xl * 2 + core

    def tile_id(step):
        t = lax.rem(me + step, NT)
        return t, {"blk_0": t // 32, "blk_1": lax.rem(t // 8, 4), "blk_2": lax.rem(t, 8)}

    def chan_id(step):
        c = lax.rem(quarter + step, 4)
        return c, {"chan_0": c // 2, "chan_1": lax.rem(c, 2)}

    def x_id(step):
        other = lax.rem(x + step, 4)
        return other, {"blk_0": other // 2, "chan_0": lax.rem(other, 2)}

    barrier = pltpu.get_barrier_semaphore()

    def greet(step, carry):
        pl.semaphore_signal(barrier, inc=1, device_id=tile_id(step)[1], device_id_type=MESH)
        return carry

    lax.fori_loop(1, NT, greet, 0)
    for step in range(1, 4):
        pl.semaphore_signal(barrier, inc=1, device_id=chan_id(step)[1], device_id_type=MESH)
        pl.semaphore_signal(barrier, inc=1, device_id=x_id(step)[1], device_id_type=MESH)
    pl.semaphore_wait(barrier, NT - 1 + 6)

    def remote(src, dst, k, device):
        return pltpu.make_async_remote_copy(
            src_ref=src,
            dst_ref=dst,
            send_sem=send_sem.at[k],
            recv_sem=recv_sem.at[k],
            device_id=device,
            device_id_type=MESH,
        )

    for step in range(1, 4):
        c, device = chan_id(step)
        remote(pq_ref.at[c], part.at[step - 1], step - 1, device).start()

    def send_tile(step, carry):
        t, device = tile_id(step)
        pltpu.make_async_remote_copy(
            src_ref=rows_ref.at[t], dst_ref=got_rows.at[me], send_sem=a2a_send.at[0],
            recv_sem=a2a_recv.at[0], device_id=device, device_id_type=MESH,
        ).start()
        pltpu.make_async_remote_copy(
            src_ref=ints_ref.at[t], dst_ref=got_ints.at[me], send_sem=a2a_send.at[1],
            recv_sem=a2a_recv.at[1], device_id=device, device_id_type=MESH,
        ).start()
        return carry

    total = pq_ref[quarter]
    for step in range(1, 4):
        c, device = chan_id(step)
        remote(pq_ref.at[c], part.at[step - 1], step - 1, device).wait()
        total = total + part[step - 1]
    total = jnp.concatenate([total[:6], pq_ref[0, 6:8, :]], axis=0)
    mine = jnp.concatenate([total[:, :128], total[:, 128:]], axis=0).astype(BF16)
    all_ref[core, x, y, z] = mine

    for step in range(1, 8):
        remote(all_ref.at[core, x, y, z], all_ref.at[core, x, y, z], 3, {"blk_2": lax.rem(z + step, 8)}).start()
    lax.fori_loop(1, NT, send_tile, 0)
    keep_rows = pltpu.make_async_copy(rows_ref.at[me], got_rows.at[me], own_sem.at[0])
    keep_ints = pltpu.make_async_copy(ints_ref.at[me], got_ints.at[me], own_sem.at[1])
    keep_rows.start()
    keep_ints.start()
    line = all_ref.at[core, x, y, pl.ds(0, 7)]
    remote(line, line, 3, {"blk_2": lax.rem(z + 1, 8)}).wait()

    plane = all_ref.at[core, x, y]
    for step in range(1, 4):
        remote(plane, plane, 4, {"blk_1": lax.rem(y + step, 4)}).start()
    span = all_ref.at[core, x, pl.ds(0, 3)]
    remote(span, span, 4, {"blk_1": lax.rem(y + 1, 4)}).wait()

    slab = all_ref.at[core, x]
    for step in range(1, 4):
        remote(slab, slab, 5, x_id(step)[1]).start()
    span = all_ref.at[core, pl.ds(0, 3)]
    remote(span, span, 5, x_id(1)[1]).wait()

    half = all_ref.at[core]
    other = {"chan_1": 1 - core}
    copy = remote(half, half, 6, other)
    copy.start()
    copy.wait()

    keep_rows.wait()
    keep_ints.wait()
    for buf, k in ((got_rows, 0), (got_ints, 1)):
        span = buf.at[pl.ds(0, NT - 1)]
        pltpu.make_async_remote_copy(
            src_ref=span, dst_ref=span, send_sem=a2a_send.at[k],
            recv_sem=a2a_recv.at[k], device_id=other, device_id_type=MESH,
        ).wait()


def exchange(pq, rows, ints):
    return pl.pallas_call(
        exchange_kernel,
        name="exchange",
        out_shape=(
            jax.ShapeDtypeStruct((2, 4, 4, 8, 16, 128), BF16),
            jax.ShapeDtypeStruct((NT, 8, 128), BF16),
            jax.ShapeDtypeStruct((NT, 4, 128), I32),
        ),
        in_specs=[VM, VM, VM],
        out_specs=(VM, VM, VM),
        scratch_shapes=[
            pltpu.VMEM((3, 8, 256), F32),
            pltpu.SemaphoreType.DMA((7,)),
            pltpu.SemaphoreType.DMA((7,)),
            pltpu.SemaphoreType.DMA((2,)),
            pltpu.SemaphoreType.DMA((2,)),
            pltpu.SemaphoreType.DMA((2,)),
        ],
        compiler_params=pltpu.CompilerParams(collective_id=0, has_side_effects=True),
    )(pq, rows, ints)


def solve(wide_ref, gain_ref, p_refs):
    def lines(core, xl, half, slot, part):
        out = []
        for xh in range(2):
            group = core * 4 + xh * 2 + xl
            out.append(wide_ref[pl.ds(group * 512 + half * 8 + slot * 3 + part, 32, stride=16), :])
        return out

    for core in range(2):
        for xl in range(2):
            for half in range(2):
                tb = (xl * 2 + core) * 2 + half
                for part in range(3):
                    block = lines(core, xl, half, 0, part) + lines(core, xl, half, 1, part)
                    p_refs[part][tb * 128 : tb * 128 + 128, :] = jnp.concatenate(block, axis=0).T

    def pair_lines(side):
        out = []
        for slot in range(2):
            for xh in range(2):
                out.append(wide_ref[pl.ds((xh * 2) * 512 + slot * 8 + 6 + side, 32, stride=16), :])
        return out

    lane = iota((128, 128), 1).astype(F32)
    blocks = [pair_lines(0), pair_lines(1)]
    columns = [jnp.concatenate(b, axis=0) for b in blocks]
    onehot = jnp.concatenate([(c == lane).astype(F32) for c in columns], axis=0)
    rows = [c.T[:32].astype(I32) for c in columns]

    def spread(g, which):
        return jnp.take_along_axis(g, rows[which], axis=1)

    pr_ref, pi_ref, q_ref = p_refs
    gr = gain_ref[0]
    gi = gain_ref[1]
    for sweep in range(ITERS):
        ar, ai, br, bi = spread(gr, 0), spread(gi, 0), spread(gr, 1), spread(gi, 1)
        a2 = ar * ar + ai * ai
        b2 = br * br + bi * bi
        zero = jnp.zeros((32, 128), F32)
        first = [zero, zero, zero]
        second = [zero, zero, zero]
        for i in range(32):
            pr = pr_ref[i * 32 : i * 32 + 32, :]
            pi = pi_ref[i * 32 : i * 32 + 32, :]
            q = q_ref[i * 32 : i * 32 + 32, :]
            xr, xi, x2 = ar[i : i + 1], ai[i : i + 1], a2[i : i + 1]
            second[0] = second[0] + (pr * xr + pi * xi)
            second[1] = second[1] + (pr * xi - pi * xr)
            second[2] = second[2] + q * x2
        for j in range(32):
            at = pl.ds(j, 32, stride=32)
            pr, pi, q = pr_ref[at, :], pi_ref[at, :], q_ref[at, :]
            xr, xi, x2 = br[j : j + 1], bi[j : j + 1], b2[j : j + 1]
            first[0] = first[0] + (pr * xr - pi * xi)
            first[1] = first[1] + (pr * xi + pi * xr)
            first[2] = first[2] + q * x2
        terms = jnp.concatenate([jnp.concatenate(first, axis=0), jnp.concatenate(second, axis=0)], axis=1)
        total = jnp.dot(terms, onehot, precision=lax.Precision.HIGHEST, preferred_element_type=F32)
        denominator = jnp.where(iota((32, 128), 1) < NB, total[64:96], 1.0)
        ur = total[0:32] / denominator
        ui = total[32:64] / denominator
        if sweep % 2 == 1:
            gr, gi = 0.5 * (ur + gr), 0.5 * (ui + gi)
        else:
            gr, gi = ur, ui
    return gr, gi


def residual_rows(gr, gi, wide_ref, lines_ref, ints_ref, res_ref):
    turned_r = gr.T[:NB, :]
    turned_i = gi.T[:NB, :]
    turned_r = jnp.concatenate([turned_r] * 4, axis=1)
    turned_i = jnp.concatenate([turned_i] * 4, axis=1)

    def blocks(slot, side):
        return jnp.concatenate(
            [wide_ref[pl.ds((xh * 2) * 512 + slot * 8 + 6 + side, 32, stride=16), :] for xh in range(2)], axis=0
        )

    lane = iota((NT, 128), 1)
    which = jnp.where(
        lane < 64,
        jnp.where(lane < 32, blocks(0, 0), blocks(1, 0)),
        jnp.where(lane < 96, blocks(0, 1), blocks(1, 1)),
    ).astype(I32)
    table_r = jnp.zeros((NT, 128), F32)
    table_i = jnp.zeros((NT, 128), F32)
    for n in range(NB):
        hit = which == n
        table_r = jnp.where(hit, turned_r[n : n + 1], table_r)
        table_i = jnp.where(hit, turned_i[n : n + 1], table_i)
    for half in range(2):
        place = ints_ref[pl.ds(2 + half, NT, stride=4), :]
        slot = (place >> 10) * 32
        at_a = slot + ((place >> 5) & 31)
        at_b = slot + (place & 31) + 64
        ar = jnp.take_along_axis(table_r, at_a, axis=1)
        ai = jnp.take_along_axis(table_i, at_a, axis=1)
        br = jnp.take_along_axis(table_r, at_b, axis=1)
        bi = jnp.take_along_axis(table_i, at_b, axis=1)
        vr, vi, mr, mi = (lines_ref[pl.ds(q * 2 + half, NT, stride=8), :] for q in range(4))
        twisted_r = mr * br + mi * bi
        twisted_i = mi * br - mr * bi
        res_ref[0, half] = (vr - (ar * twisted_r - ai * twisted_i)).astype(BF16).astype(F32)
        res_ref[1, half] = (vi - (ar * twisted_i + ai * twisted_r)).astype(BF16).astype(F32)


def window(code):
    shifted = iota((8, 128), 0) * 8 - code
    block = (32 - shifted) >> 6
    distance = block * 64 + shifted
    angle = distance.astype(F32) * (math.pi / 64)
    z = angle * angle
    cos = 1.0 / math.factorial(14)
    for k in range(6, -1, -1):
        cos = 1.0 / math.factorial(2 * k) - z * cos
    value = jnp.where(jnp.abs(distance) < 32, cos * cos, 0.0).astype(BF16).astype(F32)
    return block, value


def owner_kernel(all_ref, rows_ref, ints_ref, gain_ref, grid_ref, solved_ref, wide_ref, pr_ref, pi_ref, q_ref, lines_ref, res_ref):
    wide_ref[...] = all_ref[...].astype(F32)
    lines_ref[...] = rows_ref[...].astype(F32)
    gr, gi = solve(wide_ref, gain_ref, (pr_ref, pi_ref, q_ref))
    solved_ref[0] = gr.T[:NB, :]
    solved_ref[1] = gi.T[:NB, :]
    residual_rows(gr, gi, wide_ref, lines_ref, ints_ref, res_ref)

    def step(group, acc):
        lefts, rights = [], []
        for member in range(4):
            s = group * 4 + member
            for half in range(2):
                both = ints_ref[pl.ds(s * 4 + half, 1), :]
                ublock, uvalue = window(both & 65535)
                vblock, vvalue = window(both >> 16)
                hr = (vvalue * res_ref[0, half, pl.ds(s, 1), :]).astype(BF16).astype(F32)
                hi = (vvalue * res_ref[1, half, pl.ds(s, 1), :]).astype(BF16).astype(F32)
                lefts.append(
                    jnp.concatenate([jnp.where(ublock == k, uvalue, 0.0) for k in range(16)], axis=0).astype(BF16)
                )
                hits = [vblock == k for k in range(16)]
                rights.append(
                    jnp.concatenate(
                        [jnp.where(hit, hr, 0.0) for hit in hits] + [jnp.where(hit, hi, 0.0) for hit in hits], axis=0
                    ).astype(BF16)
                )
        left = jnp.concatenate(lefts, axis=1)
        right = jnp.concatenate(rights, axis=1)
        return acc + lax.dot_general(left, right, (((1,), (1,)), ((), ())), preferred_element_type=F32)

    acc = lax.fori_loop(0, NT // 4, step, jnp.zeros((TS, 2 * TS), F32))
    grid_ref[0] = acc[:, :TS]
    grid_ref[1] = acc[:, TS:]


def owner(everything, rows, ints, gains):
    return pl.pallas_call(
        owner_kernel,
        name="owner",
        out_shape=(
            jax.ShapeDtypeStruct((2, TS, TS), F32),
            jax.ShapeDtypeStruct((2, NB, BS), F32),
        ),
        in_specs=[VM, VM, VM, VM],
        out_specs=(VM, VM),
        scratch_shapes=[
            pltpu.VMEM((4096, 128), F32),
            pltpu.VMEM((1024, 128), F32),
            pltpu.VMEM((1024, 128), F32),
            pltpu.VMEM((1024, 128), F32),
            pltpu.VMEM((512, 128), F32),
            pltpu.VMEM((2, 2, NT, 128), F32),
        ],
    )(everything.reshape(4096, 128), rows.reshape(512, 128), ints.reshape(256, 128), gains)


def start_gains(gain_amp, gain_phase):
    both = jnp.stack((gain_amp * jnp.cos(gain_phase), gain_amp * jnp.sin(gain_phase)))
    turned = both.reshape(2, NB, BS).transpose(0, 2, 1)
    return jnp.pad(turned, ((0, 0), (0, 0), (0, 128 - NB)))


def shards(pair_map, visibilities, model_vis, flag_mask, gain_amp, gain_phase, row_index, cell_codes):
    gains = start_gains(gain_amp, gain_phase)
    pq, rows, ints = sender(
        pair_map, visibilities, model_vis, flag_mask, row_index[0, 0], cell_codes.reshape(2, NT, 256)
    )
    everything, got_rows, got_ints = exchange(pq, rows, ints)
    grid, solved = owner(everything, got_rows, got_ints, gains)
    return grid[None, None], solved.reshape(2, S)


def solution(mesh):
    split = Mesh(mesh.devices.reshape(2, 4, 8, 2, 2), BLK + CHAN)
    placed = (
        P(BLK, None),
        P(None, BLK, CHAN, None),
        P(None, BLK, CHAN, None),
        P(BLK, CHAN, None),
        P(),
        P(),
        P(CHAN, BLK, None, None),
        P(None, CHAN, BLK, None, None),
    )
    return jax.shard_map(
        shards,
        mesh=split,
        in_specs=placed,
        out_specs=(P(CHAN, BLK, None, None, None), P()),
        check_vma=False,
    )
```

```python
import math

import jax
import jax.numpy as jnp
from jax import lax
from jax.experimental import pallas as pl
from jax.experimental.pallas import tpu as pltpu
from jax.sharding import Mesh
from jax.sharding import PartitionSpec as P

S = 512
BS = 32
NB = 16
ITERS = 3
TS = 128
NT = 64
CH = 16
F32 = jnp.float32
BF16 = jnp.bfloat16
I32 = jnp.int32
MESH = pl.DeviceIdType.MESH
BLK = ("blk_0", "blk_1", "blk_2")
CHAN = ("chan_0", "chan_1")
VM = pl.BlockSpec(memory_space=pltpu.VMEM)
SM = pl.BlockSpec(memory_space=pltpu.SMEM)


def iota(shape, axis):
    return lax.broadcasted_iota(I32, shape, axis)


def sums_and_tables(pm_ref, vis_ref, mod_ref, flag_ref, pq_ref, table_ref):
    for slot in range(2):
        first = pm_ref[slot, 0]
        second = pm_ref[slot, 1]
        same = (first == second).astype(F32)
        lane = iota((1, 128), 1)
        planes = [[], [], [], []]
        for tb in range(8):
            at = slice(tb * 128, tb * 128 + 128)
            base = lane + tb * 128
            diagonal = ((base >> 5) == (base & 31)).astype(F32)
            weight = flag_ref[slot, :, at].astype(F32) * (1.0 - same * diagonal)
            vr = vis_ref[0, slot, :, at].astype(F32) * weight
            vi = vis_ref[1, slot, :, at].astype(F32) * weight
            mr = mod_ref[0, slot, :, at].astype(F32) * weight
            mi = mod_ref[1, slot, :, at].astype(F32) * weight
            sums = (
                jnp.sum(vr * mr + vi * mi, axis=0, keepdims=True),
                jnp.sum(vi * mr - vr * mi, axis=0, keepdims=True),
                jnp.sum(mr * mr + mi * mi, axis=0, keepdims=True),
            )
            col = slice((tb % 2) * 128, (tb % 2) * 128 + 128)
            for q in range(3):
                row = slot * 3 + q
                pq_ref[tb // 2, row : row + 1, col] = sums[q]
            for plane, value in zip(planes, (vr, vi, mr, mi)):
                plane.append(value)
        for q in range(4):
            table = jnp.concatenate(planes[q], axis=0)
            table_ref[q * 128 : q * 128 + 128, slot * 128 : slot * 128 + 128] = table.T.astype(BF16)
        for quarter in range(4):
            col = slice(slot * 128, slot * 128 + 128)
            pq_ref[quarter, 6:7, col] = jnp.full((1, 128), first.astype(F32))
            pq_ref[quarter, 7:8, col] = jnp.full((1, 128), second.astype(F32))


def iota_table():
    return iota((256, 256), 0).astype(F32).astype(BF16)


def gather_tile(tile, index_ref, codes_ref, table_ref, iota_ref, rows_ref):
    index = index_ref[pl.ds(tile, 1), :]
    hi = ((index >> 14) << 7) | (((index >> 7) & 7) << 4) | ((index >> 10) & 15)
    high = jnp.broadcast_to(hi.astype(F32), (16, 256)).astype(BF16)
    one, zero = jnp.ones((16, 256), BF16), jnp.zeros((16, 256), BF16)
    onehot = jnp.concatenate(
        [jnp.where(iota_ref[k * 16 : k * 16 + 16, :] == high, one, zero) for k in range(16)], axis=0
    )
    lifted = jnp.dot(table_ref[...], onehot, preferred_element_type=F32)
    low_high = (index >> 3) & 15
    live = iota((8, 256), 0) == (index & 7)
    masks = [jnp.broadcast_to(low_high == k, (8, 256)) for k in range(16)]
    pieces = []
    for q in range(4):
        part = lifted[q * 128 : q * 128 + 8]
        for k in range(1, 16):
            part = jnp.where(masks[k], lifted[q * 128 + k * 8 : q * 128 + k * 8 + 8], part)
        value = jnp.sum(jnp.where(live, part, 0.0), axis=0, keepdims=True)
        pieces += [value[:, :128], value[:, 128:]]
    rows_ref[tile] = jnp.concatenate(pieces, axis=0).astype(BF16)


def write_ints(tile, index_ref, codes_ref, ints_ref):
    index = index_ref[pl.ds(tile, 1), :]
    both = codes_ref[0, pl.ds(tile, 1), :] | (codes_ref[1, pl.ds(tile, 1), :] << 16)
    place = (((index >> 14) & 1) << 10) | (index & 1023)
    ints_ref[tile] = jnp.concatenate([both[:, :128], both[:, 128:], place[:, :128], place[:, 128:]], axis=0)


NEAR = (1, 3, 2)


def front_kernel(
    pm_ref, vis_ref, mod_ref, flag_ref, index_ref, codes_ref,
    all_ref, got_rows, got_ints,
    table_ref, iota_ref, pq_ref, rows_ref, ints_ref, part,
    sum_send, sum_recv, line_send, line_recv, in_send, in_recv, out_send, out_recv,
    core_send, core_recv, a2a_send, a2a_recv, own_sem,
):
    xh, y, z = lax.axis_index("blk_0"), lax.axis_index("blk_1"), lax.axis_index("blk_2")
    xl, core = lax.axis_index("chan_0"), lax.axis_index("chan_1")
    me = (xh * 4 + y) * 8 + z
    x = xh * 2 + xl
    quarter = xl * 2 + core
    inner = y * (1 - core) + x * core
    outer = x * (1 - core) + y * core

    def tile_id(step):
        t = lax.rem(me + step, NT)
        return t, {"blk_0": t // 32, "blk_1": lax.rem(t // 8, 4), "blk_2": lax.rem(t, 8)}

    def chan_id(step):
        c = lax.rem(quarter + step, 4)
        return c, {"chan_0": c // 2, "chan_1": lax.rem(c, 2)}

    def plane_id(in_step, out_step):
        i, o = lax.rem(inner + in_step, 4), lax.rem(outer + out_step, 4)
        py = i * (1 - core) + o * core
        px = o * (1 - core) + i * core
        return {"blk_0": px // 2, "chan_0": lax.rem(px, 2), "blk_1": py}

    barrier = pltpu.get_barrier_semaphore()

    def greet(step, carry):
        pl.semaphore_signal(barrier, inc=1, device_id=tile_id(step)[1], device_id_type=MESH)
        return carry

    for step in range(1, 4):
        pl.semaphore_signal(barrier, inc=1, device_id=chan_id(step)[1], device_id_type=MESH)
        pl.semaphore_signal(
            barrier, inc=1, device_id={"blk_0": lax.rem(x + step, 4) // 2, "chan_0": lax.rem(x + step, 2)},
            device_id_type=MESH,
        )
    lax.fori_loop(1, NT, greet, 0)

    def remote(src, dst, send, recv, device):
        return pltpu.make_async_remote_copy(
            src_ref=src, dst_ref=dst, send_sem=send, recv_sem=recv, device_id=device, device_id_type=MESH
        )

    def gather(first, last):
        def step(group, carry):
            for member in range(4):
                gather_tile(group * 4 + member, index_ref, codes_ref, table_ref, iota_ref, rows_ref)
            return carry

        lax.fori_loop(first // 4, last // 4, step, 0)

    def to_owners(src, dst, k):
        def step(n, carry):
            t, device = tile_id(n)
            remote(src.at[t], dst.at[me], a2a_send.at[k], a2a_recv.at[k], device).start()
            return carry

        lax.fori_loop(1, NT, step, 0)

    sums_and_tables(pm_ref, vis_ref, mod_ref, flag_ref, pq_ref, table_ref)
    iota_ref[...] = iota_table()

    def ints_step(group, carry):
        for member in range(4):
            write_ints(group * 4 + member, index_ref, codes_ref, ints_ref)
        return carry

    lax.fori_loop(0, NT // 4, ints_step, 0)
    gather(0, CUT[0])
    pl.semaphore_wait(barrier, NT - 1 + 6)

    def piece(step):
        c, device = chan_id(step)
        return remote(pq_ref.at[c], part.at[step - 1], sum_send.at[step - 1], sum_recv.at[step - 1], device)

    for step in range(1, 4):
        piece(step).start()
    to_owners(ints_ref, got_ints, 1)
    keep_ints = pltpu.make_async_copy(ints_ref.at[me], got_ints.at[me], own_sem.at[1])
    keep_ints.start()
    gather(CUT[0], CUT[1])
    total = pq_ref[quarter]
    for step in range(1, 4):
        piece(step).wait_recv()
        total = total + part[step - 1]
    total = jnp.concatenate([total[:6], pq_ref[0, 6:8, :]], axis=0)
    all_ref[core, outer, inner, z] = jnp.concatenate([total[:, :128], total[:, 128:]], axis=0).astype(BF16)

    mine = all_ref.at[core, outer, inner, z]
    for step in range(1, 8):
        remote(mine, mine, line_send.at[0], line_recv.at[0], {"blk_2": lax.rem(z + step, 8)}).start()
    gather(CUT[1], NT)
    to_owners(rows_ref, got_rows, 0)
    keep_rows = pltpu.make_async_copy(rows_ref.at[me], got_rows.at[me], own_sem.at[0])
    keep_rows.start()
    seven = all_ref.at[core, outer, inner, pl.ds(0, 7)]
    line = remote(seven, seven, line_send.at[0], line_recv.at[0], {"blk_2": lax.rem(z + 1, 8)})
    line.wait_recv()

    def block(back):
        return all_ref.at[core, outer, lax.rem(inner + 4 - back, 4)]

    def inward(step):
        src = block(0)
        return remote(src, src, in_send.at[step - 1], in_recv.at[step - 1], plane_id(step, 0))

    def outward(back, step):
        src = block(back)
        return remote(src, src, out_send.at[back, step - 1], out_recv.at[back, step - 1], plane_id(0, step))

    for step in NEAR:
        inward(step).start()
    for step in NEAR:
        outward(0, step).start()
    for back in NEAR:
        inward(back).wait_recv()
        for step in NEAR:
            outward(back, step).start()

    def across(back):
        src = all_ref.at[core, lax.rem(outer + 4 - back, 4)]
        return remote(src, src, core_send.at[back], core_recv.at[back], {"chan_1": 1 - core})

    across(0).start()
    for step in NEAR:
        for back in (0,) + NEAR:
            outward(back, step).wait_recv()
        across(step).start()

    for step in range(4):
        across(step).wait_recv()
    keep_rows.wait()
    keep_ints.wait()
    for buf, k in ((got_rows, 0), (got_ints, 1)):
        span = buf.at[pl.ds(0, NT - 1)]
        remote(span, span, a2a_send.at[k], a2a_recv.at[k], {"chan_1": 1 - core}).wait()
    for step in range(1, 4):
        piece(step).wait_send()
        inward(step).wait_send()
        for back in range(4):
            outward(back, step).wait_send()
    line.wait_send()
    for step in range(4):
        across(step).wait_send()


CUT = (28, 52)


def front(pm, vis, mod, flag, index, codes):
    dma = pltpu.SemaphoreType.DMA
    return pl.pallas_call(
        front_kernel,
        name="front",
        out_shape=(
            jax.ShapeDtypeStruct((2, 4, 4, 8, 16, 128), BF16),
            jax.ShapeDtypeStruct((NT, 8, 128), BF16),
            jax.ShapeDtypeStruct((NT, 4, 128), I32),
        ),
        in_specs=[SM, VM, VM, VM, VM, VM],
        out_specs=(VM, VM, VM),
        scratch_shapes=[
            pltpu.VMEM((512, 256), BF16),
            pltpu.VMEM((256, 256), BF16),
            pltpu.VMEM((4, 8, 256), F32),
            pltpu.VMEM((NT, 8, 128), BF16),
            pltpu.VMEM((NT, 4, 128), I32),
            pltpu.VMEM((3, 8, 256), F32),
            dma((3,)), dma((3,)), dma((1,)), dma((1,)), dma((3,)), dma((3,)), dma((4, 3)), dma((4, 3)),
            dma((4,)), dma((4,)), dma((2,)), dma((2,)), dma((2,)),
        ],
        compiler_params=pltpu.CompilerParams(collective_id=0, has_side_effects=True),
    )(pm, vis, mod, flag, index, codes)


def wide_lines(wide_ref, core, xl, row):
    out = []
    for xh in range(2):
        for y in range(4):
            x = xh * 2 + xl
            place = (x * 4 + y) if core == 0 else (16 + y * 4 + x)
            out.append(wide_ref[pl.ds(place * 128 + row, 8, stride=16), :])
    return out


def block_row(block):
    n = block.astype(I32)
    return ((n & 3) << 2) | (n >> 2)


def start_gains(amp_ref, phase_ref):
    amp, phase = amp_ref[...], phase_ref[...]
    out = []
    for value in (amp * jnp.cos(phase), amp * jnp.sin(phase)):
        stacked = jnp.concatenate([value[:, a * 32 : a * 32 + 32] for a in range(4)], axis=0)
        stacked = jnp.concatenate([stacked, jnp.zeros((112, 32), F32)], axis=0)
        out.append(stacked.T)
    return out


def solve(wide_ref, amp_ref, phase_ref, p_refs):
    for core in range(2):
        for xl in range(2):
            for half in range(2):
                tb = (xl * 2 + core) * 2 + half
                for part in range(3):
                    block = []
                    for slot in range(2):
                        block += wide_lines(wide_ref, core, xl, half * 8 + slot * 3 + part)
                    p_refs[part][tb * 128 : tb * 128 + 128, :] = jnp.concatenate(block, axis=0).T

    lane = iota((128, 128), 1)
    columns = []
    for side in range(2):
        block = []
        for slot in range(2):
            block += wide_lines(wide_ref, 0, 0, slot * 8 + 6 + side)
        columns.append(block_row(jnp.concatenate(block, axis=0)))
    onehot = jnp.concatenate([(c == lane).astype(F32) for c in columns], axis=0)
    rows = [c.astype(F32).T[:32].astype(I32) for c in columns]

    def spread(g, which):
        return jnp.take_along_axis(g, rows[which], axis=1)

    pr_ref, pi_ref, q_ref = p_refs
    gr, gi = start_gains(amp_ref, phase_ref)
    for sweep in range(ITERS):
        ar, ai, br, bi = spread(gr, 0), spread(gi, 0), spread(gr, 1), spread(gi, 1)
        a2 = ar * ar + ai * ai
        b2 = br * br + bi * bi
        zero = jnp.zeros((32, 128), F32)
        first = [zero, zero, zero]
        second = [zero, zero, zero]
        for i in range(32):
            pr = pr_ref[i * 32 : i * 32 + 32, :]
            pi = pi_ref[i * 32 : i * 32 + 32, :]
            q = q_ref[i * 32 : i * 32 + 32, :]
            xr, xi, x2 = ar[i : i + 1], ai[i : i + 1], a2[i : i + 1]
            second[0] = second[0] + (pr * xr + pi * xi)
            second[1] = second[1] + (pr * xi - pi * xr)
            second[2] = second[2] + q * x2
        for j in range(32):
            at = pl.ds(j, 32, stride=32)
            pr, pi, q = pr_ref[at, :], pi_ref[at, :], q_ref[at, :]
            xr, xi, x2 = br[j : j + 1], bi[j : j + 1], b2[j : j + 1]
            first[0] = first[0] + (pr * xr - pi * xi)
            first[1] = first[1] + (pr * xi + pi * xr)
            first[2] = first[2] + q * x2
        terms = jnp.concatenate([jnp.concatenate(first, axis=0), jnp.concatenate(second, axis=0)], axis=1)
        total = jnp.dot(terms, onehot, precision=lax.Precision.HIGHEST, preferred_element_type=F32)
        denominator = jnp.where(iota((32, 128), 1) < NB, total[64:96], 1.0)
        ur = total[0:32] / denominator
        ui = total[32:64] / denominator
        if sweep % 2 == 1:
            gr, gi = 0.5 * (ur + gr), 0.5 * (ui + gi)
        else:
            gr, gi = ur, ui
    return gr, gi


def residual_rows(gr, gi, wide_ref, lines_ref, ints_ref, res_ref):
    turned_r = gr.T[:NB, :]
    turned_i = gi.T[:NB, :]
    turned_r = jnp.concatenate([turned_r] * 4, axis=1)
    turned_i = jnp.concatenate([turned_i] * 4, axis=1)

    def blocks(slot, side):
        return block_row(jnp.concatenate(wide_lines(wide_ref, 0, 0, slot * 8 + 6 + side), axis=0))

    lane = iota((NT, 128), 1)
    which = jnp.where(
        lane < 64,
        jnp.where(lane < 32, blocks(0, 0), blocks(1, 0)),
        jnp.where(lane < 96, blocks(0, 1), blocks(1, 1)),
    )
    table_r = jnp.zeros((NT, 128), F32)
    table_i = jnp.zeros((NT, 128), F32)
    for n in range(NB):
        hit = which == n
        table_r = jnp.where(hit, turned_r[n : n + 1], table_r)
        table_i = jnp.where(hit, turned_i[n : n + 1], table_i)
    for half in range(2):
        place = ints_ref[pl.ds(2 + half, NT, stride=4), :]
        slot = (place >> 10) * 32
        at_a = slot + ((place >> 5) & 31)
        at_b = slot + (place & 31) + 64
        ar = jnp.take_along_axis(table_r, at_a, axis=1)
        ai = jnp.take_along_axis(table_i, at_a, axis=1)
        br = jnp.take_along_axis(table_r, at_b, axis=1)
        bi = jnp.take_along_axis(table_i, at_b, axis=1)
        vr, vi, mr, mi = (lines_ref[pl.ds(q * 2 + half, NT, stride=8), :] for q in range(4))
        twisted_r = mr * br + mi * bi
        twisted_i = mi * br - mr * bi
        res_ref[0, half] = (vr - (ar * twisted_r - ai * twisted_i)).astype(BF16).astype(F32)
        res_ref[1, half] = (vi - (ar * twisted_i + ai * twisted_r)).astype(BF16).astype(F32)


def window(code):
    shifted = iota((8, 128), 0) * 8 - code
    block = (32 - shifted) >> 6
    distance = block * 64 + shifted
    angle = distance.astype(F32) * (math.pi / 64)
    z = angle * angle
    cos = 1.0 / math.factorial(14)
    for k in range(6, -1, -1):
        cos = 1.0 / math.factorial(2 * k) - z * cos
    value = jnp.where(jnp.abs(distance) < 32, cos * cos, 0.0).astype(BF16).astype(F32)
    return block, value


def owner_kernel(all_ref, rows_ref, ints_ref, amp_ref, phase_ref, grid_ref, solved_ref, wide_ref, pr_ref, pi_ref, q_ref, lines_ref, res_ref):
    wide_ref[...] = all_ref[...].astype(F32)
    lines_ref[...] = rows_ref[...].astype(F32)
    gr, gi = solve(wide_ref, amp_ref, phase_ref, (pr_ref, pi_ref, q_ref))
    for part, g in enumerate((gr, gi)):
        turned = g.T
        at = [(n % 4) * 4 + n // 4 for n in range(NB)]
        solved_ref[part : part + 1, :] = jnp.concatenate([turned[n : n + 1, :] for n in at], axis=1)
    residual_rows(gr, gi, wide_ref, lines_ref, ints_ref, res_ref)

    def step(group, acc):
        lefts, rights = [], []
        for member in range(4):
            s = group * 4 + member
            for half in range(2):
                both = ints_ref[pl.ds(s * 4 + half, 1), :]
                ublock, uvalue = window(both & 65535)
                vblock, vvalue = window(both >> 16)
                hr = (vvalue * res_ref[0, half, pl.ds(s, 1), :]).astype(BF16).astype(F32)
                hi = (vvalue * res_ref[1, half, pl.ds(s, 1), :]).astype(BF16).astype(F32)
                lefts.append(
                    jnp.concatenate([jnp.where(ublock == k, uvalue, 0.0) for k in range(16)], axis=0).astype(BF16)
                )
                hits = [vblock == k for k in range(16)]
                rights.append(
                    jnp.concatenate(
                        [jnp.where(hit, hr, 0.0) for hit in hits] + [jnp.where(hit, hi, 0.0) for hit in hits], axis=0
                    ).astype(BF16)
                )
        left = jnp.concatenate(lefts, axis=1)
        right = jnp.concatenate(rights, axis=1)
        return acc + lax.dot_general(left, right, (((1,), (1,)), ((), ())), preferred_element_type=F32)

    acc = lax.fori_loop(0, NT // 4, step, jnp.zeros((TS, 2 * TS), F32))
    grid_ref[0] = acc[:, :TS]
    grid_ref[1] = acc[:, TS:]


def owner(everything, rows, ints, amp, phase):
    return pl.pallas_call(
        owner_kernel,
        name="owner",
        out_shape=(
            jax.ShapeDtypeStruct((2, TS, TS), F32),
            jax.ShapeDtypeStruct((2, S), F32),
        ),
        in_specs=[VM] * 5,
        out_specs=(VM, VM),
        scratch_shapes=[
            pltpu.VMEM((4096, 128), F32),
            pltpu.VMEM((1024, 128), F32),
            pltpu.VMEM((1024, 128), F32),
            pltpu.VMEM((1024, 128), F32),
            pltpu.VMEM((512, 128), F32),
            pltpu.VMEM((2, 2, NT, 128), F32),
        ],
    )(everything.reshape(4096, 128), rows.reshape(512, 128), ints.reshape(256, 128), amp.reshape(4, 128), phase.reshape(4, 128))


def shards(pair_map, visibilities, model_vis, flag_mask, gain_amp, gain_phase, row_index, cell_codes):
    everything, got_rows, got_ints = front(
        pair_map, visibilities, model_vis, flag_mask, row_index[0, 0], cell_codes.reshape(2, NT, 256)
    )
    grid, solved = owner(everything, got_rows, got_ints, gain_amp, gain_phase)
    return grid[None, None], solved


def solution(mesh):
    split = Mesh(mesh.devices.reshape(2, 4, 8, 2, 2), BLK + CHAN)
    placed = (
        P(BLK, None),
        P(None, BLK, CHAN, None),
        P(None, BLK, CHAN, None),
        P(BLK, CHAN, None),
        P(),
        P(),
        P(CHAN, BLK, None, None),
        P(None, CHAN, BLK, None, None),
    )
    return jax.shard_map(
        shards,
        mesh=split,
        in_specs=placed,
        out_specs=(P(CHAN, BLK, None, None, None), P()),
        check_vma=False,
    )
```

```python
import math

import jax
import jax.numpy as jnp
from jax import lax
from jax.experimental import pallas as pl
from jax.experimental.pallas import tpu as pltpu
from jax.sharding import Mesh
from jax.sharding import PartitionSpec as P

S = 512
BS = 32
NB = 16
ITERS = 3
TS = 128
NT = 64
CH = 16
F32 = jnp.float32
BF16 = jnp.bfloat16
I32 = jnp.int32
MESH = pl.DeviceIdType.MESH
BLK = ("blk_0", "blk_1", "blk_2")
CHAN = ("chan_0", "chan_1")
VM = pl.BlockSpec(memory_space=pltpu.VMEM)
SM = pl.BlockSpec(memory_space=pltpu.SMEM)


def iota(shape, axis):
    return lax.broadcasted_iota(I32, shape, axis)


def sums_and_tables(pm_ref, vis_ref, mod_ref, flag_ref, pq_ref, table_ref):
    for slot in range(2):
        first = pm_ref[slot, 0]
        second = pm_ref[slot, 1]
        same = (first == second).astype(F32)
        lane = iota((1, 128), 1)
        planes = [[], [], [], []]
        for tb in range(8):
            at = slice(tb * 128, tb * 128 + 128)
            base = lane + tb * 128
            diagonal = ((base >> 5) == (base & 31)).astype(F32)
            weight = flag_ref[slot, :, at].astype(F32) * (1.0 - same * diagonal)
            vr = vis_ref[0, slot, :, at].astype(F32) * weight
            vi = vis_ref[1, slot, :, at].astype(F32) * weight
            mr = mod_ref[0, slot, :, at].astype(F32) * weight
            mi = mod_ref[1, slot, :, at].astype(F32) * weight
            sums = (
                jnp.sum(vr * mr + vi * mi, axis=0, keepdims=True),
                jnp.sum(vi * mr - vr * mi, axis=0, keepdims=True),
                jnp.sum(mr * mr + mi * mi, axis=0, keepdims=True),
            )
            col = slice((tb % 2) * 128, (tb % 2) * 128 + 128)
            for q in range(3):
                row = slot * 3 + q
                pq_ref[tb // 2, row : row + 1, col] = sums[q]
            for plane, value in zip(planes, (vr, vi, mr, mi)):
                plane.append(value)
        for q in range(4):
            table = jnp.concatenate(planes[q], axis=0)
            table_ref[q * 128 : q * 128 + 128, slot * 128 : slot * 128 + 128] = table.T.astype(BF16)
        for quarter in range(4):
            col = slice(slot * 128, slot * 128 + 128)
            pq_ref[quarter, 6:7, col] = jnp.full((1, 128), first.astype(F32))
            pq_ref[quarter, 7:8, col] = jnp.full((1, 128), second.astype(F32))


def iota_table():
    return iota((256, 256), 0).astype(F32).astype(BF16)


def gather_tile(tile, index_ref, codes_ref, table_ref, iota_ref, rows_ref):
    index = index_ref[pl.ds(tile, 1), :]
    hi = ((index >> 14) << 7) | (((index >> 7) & 7) << 4) | ((index >> 10) & 15)
    high = jnp.broadcast_to(hi.astype(F32), (16, 256)).astype(BF16)
    one, zero = jnp.ones((16, 256), BF16), jnp.zeros((16, 256), BF16)
    onehot = jnp.concatenate(
        [jnp.where(iota_ref[k * 16 : k * 16 + 16, :] == high, one, zero) for k in range(16)], axis=0
    )
    lifted = jnp.dot(table_ref[...], onehot, preferred_element_type=F32)
    low_high = (index >> 3) & 15
    live = iota((8, 256), 0) == (index & 7)
    masks = [jnp.broadcast_to(low_high == k, (8, 256)) for k in range(16)]
    pieces = []
    for q in range(4):
        part = lifted[q * 128 : q * 128 + 8]
        for k in range(1, 16):
            part = jnp.where(masks[k], lifted[q * 128 + k * 8 : q * 128 + k * 8 + 8], part)
        value = jnp.sum(jnp.where(live, part, 0.0), axis=0, keepdims=True)
        pieces += [value[:, :128], value[:, 128:]]
    rows_ref[tile] = jnp.concatenate(pieces, axis=0).astype(BF16)


def write_ints(tile, index_ref, codes_ref, ints_ref):
    index = index_ref[pl.ds(tile, 1), :]
    both = codes_ref[0, pl.ds(tile, 1), :] | (codes_ref[1, pl.ds(tile, 1), :] << 16)
    place = (((index >> 14) & 1) << 10) | (index & 1023)
    ints_ref[tile] = jnp.concatenate([both[:, :128], both[:, 128:], place[:, :128], place[:, 128:]], axis=0)


def widen(all_ref, wide_ref, core):
    wide_ref[pl.ds(pl.multiple_of(core * 2048, 2048), 2048), :] = all_ref[core].astype(F32).reshape(2048, 128)


def wide_lines(wide_ref, core, xl, row):
    out = []
    for xh in range(2):
        for y in range(4):
            x = xh * 2 + xl
            place = core * 16 + (x * 4 + y) * (1 - core) + (y * 4 + x) * core
            out.append(wide_ref[pl.ds(place * 128 + row, 8, stride=16), :])
    return out


def turn(wide_ref, core, p_refs):
    for xl in range(2):
        for half in range(2):
            tb = (xl * 2 + core) * 2 + half
            for part in range(3):
                block = []
                for slot in range(2):
                    block += wide_lines(wide_ref, core, xl, half * 8 + slot * 3 + part)
                at = pl.ds(pl.multiple_of(tb * 128, 128), 128)
                p_refs[part][at, :] = jnp.concatenate(block, axis=0).T


def block_row(block):
    n = block.astype(I32)
    return ((n & 3) << 2) | (n >> 2)


def station_maps(wide_ref, core):
    found = []
    for side in range(2):
        for slot in range(2):
            found.append(block_row(jnp.concatenate(wide_lines(wide_ref, core, 0, slot * 8 + 6 + side), axis=0)))
    lane = iota((128, 128), 1)
    columns = [jnp.concatenate(found[:2], axis=0), jnp.concatenate(found[2:], axis=0)]
    onehot = jnp.concatenate([(c == lane).astype(F32) for c in columns], axis=0)
    rows = [c.astype(F32).T[:32].astype(I32) for c in columns]
    lane = iota((NT, 128), 1)
    which = jnp.where(
        lane < 64, jnp.where(lane < 32, found[0], found[1]), jnp.where(lane < 96, found[2], found[3])
    )
    return onehot, rows, which


def start_gains(amp_ref, phase_ref):
    amp, phase = amp_ref[...], phase_ref[...]
    out = []
    for value in (amp * jnp.cos(phase), amp * jnp.sin(phase)):
        stacked = jnp.concatenate([value[:, a * 32 : a * 32 + 32] for a in range(4)], axis=0)
        stacked = jnp.concatenate([stacked, jnp.zeros((112, 32), F32)], axis=0)
        out.append(stacked.T)
    return out


def solve(gr, gi, onehot, rows, p_refs):
    def spread(g, which):
        return jnp.take_along_axis(g, rows[which], axis=1)

    pr_ref, pi_ref, q_ref = p_refs
    for sweep in range(ITERS):
        ar, ai, br, bi = spread(gr, 0), spread(gi, 0), spread(gr, 1), spread(gi, 1)
        a2 = ar * ar + ai * ai
        b2 = br * br + bi * bi
        zero = jnp.zeros((32, 128), F32)
        first = [zero, zero, zero]
        second = [zero, zero, zero]
        for i in range(32):
            pr = pr_ref[i * 32 : i * 32 + 32, :]
            pi = pi_ref[i * 32 : i * 32 + 32, :]
            q = q_ref[i * 32 : i * 32 + 32, :]
            xr, xi, x2 = ar[i : i + 1], ai[i : i + 1], a2[i : i + 1]
            second[0] = second[0] + (pr * xr + pi * xi)
            second[1] = second[1] + (pr * xi - pi * xr)
            second[2] = second[2] + q * x2
        for j in range(32):
            at = pl.ds(j, 32, stride=32)
            pr, pi, q = pr_ref[at, :], pi_ref[at, :], q_ref[at, :]
            xr, xi, x2 = br[j : j + 1], bi[j : j + 1], b2[j : j + 1]
            first[0] = first[0] + (pr * xr - pi * xi)
            first[1] = first[1] + (pr * xi + pi * xr)
            first[2] = first[2] + q * x2
        terms = jnp.concatenate([jnp.concatenate(first, axis=0), jnp.concatenate(second, axis=0)], axis=1)
        total = jnp.dot(terms, onehot, precision=lax.Precision.HIGHEST, preferred_element_type=F32)
        denominator = jnp.where(iota((32, 128), 1) < NB, total[64:96], 1.0)
        ur = total[0:32] / denominator
        ui = total[32:64] / denominator
        if sweep % 2 == 1:
            gr, gi = 0.5 * (ur + gr), 0.5 * (ui + gi)
        else:
            gr, gi = ur, ui
    return gr, gi


def residual_rows(gr, gi, which, lines_ref, ints_ref, res_ref):
    turned_r = gr.T[:NB, :]
    turned_i = gi.T[:NB, :]
    turned_r = jnp.concatenate([turned_r] * 4, axis=1)
    turned_i = jnp.concatenate([turned_i] * 4, axis=1)

    table_r = jnp.zeros((NT, 128), F32)
    table_i = jnp.zeros((NT, 128), F32)
    for n in range(NB):
        hit = which == n
        table_r = jnp.where(hit, turned_r[n : n + 1], table_r)
        table_i = jnp.where(hit, turned_i[n : n + 1], table_i)
    for half in range(2):
        place = ints_ref[:, 2 + half, :]
        slot = (place >> 10) * 32
        at_a = slot + ((place >> 5) & 31)
        at_b = slot + (place & 31) + 64
        ar = jnp.take_along_axis(table_r, at_a, axis=1)
        ai = jnp.take_along_axis(table_i, at_a, axis=1)
        br = jnp.take_along_axis(table_r, at_b, axis=1)
        bi = jnp.take_along_axis(table_i, at_b, axis=1)
        vr, vi, mr, mi = (lines_ref[pl.ds(q * 2 + half, NT, stride=8), :] for q in range(4))
        twisted_r = mr * br + mi * bi
        twisted_i = mi * br - mr * bi
        res_ref[0, half] = (vr - (ar * twisted_r - ai * twisted_i)).astype(BF16).astype(F32)
        res_ref[1, half] = (vi - (ar * twisted_i + ai * twisted_r)).astype(BF16).astype(F32)


def window(code):
    shifted = iota((8, 128), 0) * 8 - code
    block = (32 - shifted) >> 6
    distance = block * 64 + shifted
    angle = distance.astype(F32) * (math.pi / 64)
    z = angle * angle
    cos = 1.0 / math.factorial(14)
    for k in range(6, -1, -1):
        cos = 1.0 / math.factorial(2 * k) - z * cos
    value = jnp.where(jnp.abs(distance) < 32, cos * cos, 0.0).astype(BF16).astype(F32)
    return block, value


NEAR = (1, 3, 2)
SLOT = (0, 1, 3, 5, 7, 6, 4, 2)
GROUPS = ((0, 5), (5, 3))
CUT = (20, 36, 48)


def kernel(
    pm_ref, vis_ref, mod_ref, flag_ref, index_ref, codes_ref, amp_ref, phase_ref,
    grid_ref, solved_ref,
    table_ref, iota_ref, pq_ref, rows_ref, ints_ref, part, all_ref, got_rows, got_ints,
    wide_ref, pr_ref, pi_ref, q_ref, lines_ref, res_ref, left_ref, vblock_ref, vvalue_ref,
    sum_send, sum_recv, line_send, line_recv, in_send, in_recv, out_send, out_recv,
    core_send, core_recv, a2a_send, a2a_recv, own_sem, plane_sem, far_sem,
):
    xh, y, z = lax.axis_index("blk_0"), lax.axis_index("blk_1"), lax.axis_index("blk_2")
    xl, core = lax.axis_index("chan_0"), lax.axis_index("chan_1")
    me = xh * 4 + y
    x = xh * 2 + xl
    quarter = xl * 2 + core
    inner = y * (1 - core) + x * core
    outer = x * (1 - core) + y * core

    def chan_id(step):
        c = lax.rem(quarter + step, 4)
        return c, {"chan_0": c // 2, "chan_1": lax.rem(c, 2)}

    def line_id(step):
        return {"blk_2": lax.rem(z + step, 8)}

    def y_id(step):
        return {"blk_1": lax.rem(y + step, 4)}

    def x_id(step):
        return {"blk_0": lax.rem(x + step, 4) // 2, "chan_0": lax.rem(x + step, 2)}

    def plane_id(in_step, out_step):
        i, o = lax.rem(inner + in_step, 4), lax.rem(outer + out_step, 4)
        py = i * (1 - core) + o * core
        px = o * (1 - core) + i * core
        return {"blk_0": px // 2, "chan_0": lax.rem(px, 2), "blk_1": py}

    def signal(sem, device):
        pl.semaphore_signal(sem, inc=1, device_id=device, device_id_type=MESH)

    barrier = pltpu.get_barrier_semaphore()
    for step in range(1, 4):
        signal(barrier, chan_id(step)[1])
        signal(barrier, x_id(step))
        signal(barrier, y_id(step))
    for step in range(1, 8):
        signal(barrier, line_id(step))

    def remote(src, dst, send, recv, device):
        return pltpu.make_async_remote_copy(
            src_ref=src, dst_ref=dst, send_sem=send, recv_sem=recv, device_id=device, device_id_type=MESH
        )

    def gather(first, last):
        def step(group, carry):
            for member in range(4):
                gather_tile(group * 4 + member, index_ref, codes_ref, table_ref, iota_ref, rows_ref)
            return carry

        lax.fori_loop(first // 4, last // 4, step, 0)

    def to_owners(src, dst, k):
        for away in range(8):
            tz = lax.rem(z + away, 8)
            slot = SLOT[(8 - away) % 8]

            def step(n, carry):
                line = lax.rem(me + n, 8)
                device = {"blk_0": line // 4, "blk_1": lax.rem(line, 4), "blk_2": tz}
                remote(src.at[line * 8 + tz], dst.at[me * 8 + slot], a2a_send.at[k], a2a_recv.at[k], device).start()
                return carry

            lax.fori_loop(1 if away == 0 else 0, 8, step, 0)
        keep = pltpu.make_async_copy(src.at[me * 8 + z], dst.at[me * 8], own_sem.at[k])
        keep.start()
        return keep

    def owners_done(buf, k, keep):
        span = buf.at[pl.ds(0, NT - 1)]
        remote(span, span, a2a_send.at[k], a2a_recv.at[k], {"chan_1": 1 - core}).wait()
        keep.wait()

    sums_and_tables(pm_ref, vis_ref, mod_ref, flag_ref, pq_ref, table_ref)
    pl.semaphore_wait(barrier, 16)
    for step in range(1, 4):
        signal(plane_sem, y_id(step))

    def piece(step):
        c, device = chan_id(step)
        return remote(pq_ref.at[c], part.at[step - 1], sum_send.at[step - 1], sum_recv.at[step - 1], device)

    for step in range(1, 4):
        piece(step).start()
    iota_ref[...] = iota_table()

    def ints_step(group, carry):
        for member in range(4):
            write_ints(group * 4 + member, index_ref, codes_ref, ints_ref)
        return carry

    lax.fori_loop(0, NT // 4, ints_step, 0)
    gather(0, CUT[0])
    total = pq_ref[quarter]
    for step in range(1, 4):
        piece(step).wait_recv()
        total = total + part[step - 1]
    total = jnp.concatenate([total[:6], pq_ref[0, 6:8, :]], axis=0)
    all_ref[core, outer, inner, 0] = jnp.concatenate([total[:, :128], total[:, 128:]], axis=0).astype(BF16)

    mine = all_ref.at[core, outer, inner, 0]

    def along(step):
        slot = SLOT[(8 - step) % 8]
        k = 0 if slot < 5 else 1
        return remote(mine, all_ref.at[core, outer, inner, slot], line_send.at[k], line_recv.at[k], line_id(step))

    for step in (1, 7, 2, 6, 3, 5, 4):
        along(step).start()
    pl.semaphore_wait(plane_sem, 3)
    signal(far_sem, {"blk_0": 1 - xh})
    pl.semaphore_wait(far_sem, 1)
    keep_ints = to_owners(ints_ref, got_ints, 1)
    gather(CUT[0], CUT[1])

    def line(k):
        count = (4, 3)[k]
        span = all_ref.at[core, outer, inner, pl.ds(0, count)]
        return remote(span, span, line_send.at[k], line_recv.at[k], line_id(1))

    def block(back, k):
        return all_ref.at[core, outer, lax.rem(inner + 4 - back, 4), pl.ds(*GROUPS[k])]

    def inward(step, k):
        src = block(0, k)
        return remote(src, src, in_send.at[k, step - 1], in_recv.at[k, step - 1], plane_id(step, 0))

    def outward(back, step, k):
        src = block(back, k)
        return remote(src, src, out_send.at[k, back, step - 1], out_recv.at[k, back, step - 1], plane_id(0, step))

    for k in range(2):
        line(k).wait_recv()
        for step in NEAR:
            inward(step, k).start()
        for step in NEAR:
            outward(0, step, k).start()
        if k == 0:
            gather(CUT[1], CUT[2])
    gather(CUT[2], NT)
    for k in range(2):
        for back in NEAR:
            inward(back, k).wait_recv()
            for step in NEAR:
                outward(back, step, k).start()
    keep_rows = to_owners(rows_ref, got_rows, 0)

    owners_done(got_ints, 1, keep_ints)

    def windows(s, carry):
        for half in range(2):
            both = got_ints[s, half : half + 1, :]
            ublock, uvalue = window(both & 65535)
            vblock, vvalue = window(both >> 16)
            at = pl.ds(pl.multiple_of((s * 2 + half) * 8, 8), 8)
            vblock_ref[at, :] = vblock
            vvalue_ref[at, :] = vvalue
            left_ref[:, pl.ds(pl.multiple_of((s * 2 + half) * 128, 128), 128)] = jnp.concatenate(
                [jnp.where(ublock == k, uvalue, 0.0) for k in range(16)], axis=0
            ).astype(BF16)
        return carry

    lax.fori_loop(0, NT, windows, 0)
    gr, gi = start_gains(amp_ref, phase_ref)

    def across(back):
        src = all_ref.at[core, lax.rem(outer + 4 - back, 4)]
        return remote(src, src, core_send.at[back], core_recv.at[back], {"chan_1": 1 - core})

    across(0).start()
    for step in NEAR:
        for k in range(2):
            for back in (0,) + NEAR:
                outward(back, step, k).wait_recv()
        across(step).start()

    p_refs = (pr_ref, pi_ref, q_ref)
    widen(all_ref, wide_ref, core)
    turn(wide_ref, core, p_refs)
    onehot, rows, which = station_maps(wide_ref, core)
    for step in range(4):
        across(step).wait_recv()
    widen(all_ref, wide_ref, 1 - core)
    turn(wide_ref, 1 - core, p_refs)
    gr, gi = solve(gr, gi, onehot, rows, p_refs)
    for part_at, g in enumerate((gr, gi)):
        turned = g.T
        at = [(n % 4) * 4 + n // 4 for n in range(NB)]
        solved_ref[part_at : part_at + 1, :] = jnp.concatenate([turned[n : n + 1, :] for n in at], axis=1)

    owners_done(got_rows, 0, keep_rows)
    lines_ref[...] = got_rows[...].astype(F32).reshape(512, 128)
    residual_rows(gr, gi, which, lines_ref, got_ints, res_ref)

    def grid_step(group, acc):
        rights = []
        for member in range(4):
            s = group * 4 + member
            for half in range(2):
                at = pl.ds(pl.multiple_of((s * 2 + half) * 8, 8), 8)
                vblock, vvalue = vblock_ref[at, :], vvalue_ref[at, :]
                hr = vvalue * res_ref[0, half, pl.ds(s, 1), :]
                hi = vvalue * res_ref[1, half, pl.ds(s, 1), :]
                hits = [vblock == k for k in range(16)]
                rights.append(
                    jnp.concatenate(
                        [jnp.where(hit, hr, 0.0) for hit in hits] + [jnp.where(hit, hi, 0.0) for hit in hits], axis=0
                    ).astype(BF16)
                )
        left = left_ref[:, pl.ds(pl.multiple_of(group * 1024, 1024), 1024)]
        right = jnp.concatenate(rights, axis=1)
        return acc + lax.dot_general(left, right, (((1,), (1,)), ((), ())), preferred_element_type=F32)

    acc = lax.fori_loop(0, NT // 4, grid_step, jnp.zeros((TS, 2 * TS), F32))
    grid_ref[0] = acc[:, :TS]
    grid_ref[1] = acc[:, TS:]

    for k in range(2):
        line(k).wait_send()
        for step in range(1, 4):
            inward(step, k).wait_send()
            for back in range(4):
                outward(back, step, k).wait_send()
    for step in range(1, 4):
        piece(step).wait_send()
    for step in range(4):
        across(step).wait_send()


def whole(*operands):
    dma, regular = pltpu.SemaphoreType.DMA, pltpu.SemaphoreType.REGULAR
    return pl.pallas_call(
        kernel,
        name="whole",
        out_shape=(
            jax.ShapeDtypeStruct((2, TS, TS), F32),
            jax.ShapeDtypeStruct((2, S), F32),
        ),
        in_specs=[SM] + [VM] * 7,
        out_specs=(VM, VM),
        scratch_shapes=[
            pltpu.VMEM((512, 256), BF16),
            pltpu.VMEM((256, 256), BF16),
            pltpu.VMEM((4, 8, 256), F32),
            pltpu.VMEM((NT, 8, 128), BF16),
            pltpu.VMEM((NT, 4, 128), I32),
            pltpu.VMEM((3, 8, 256), F32),
            pltpu.VMEM((2, 4, 4, 8, 16, 128), BF16),
            pltpu.VMEM((NT, 8, 128), BF16),
            pltpu.VMEM((NT, 4, 128), I32),
            pltpu.VMEM((4096, 128), F32),
            pltpu.VMEM((1024, 128), F32),
            pltpu.VMEM((1024, 128), F32),
            pltpu.VMEM((1024, 128), F32),
            pltpu.VMEM((512, 128), F32),
            pltpu.VMEM((2, 2, NT, 128), F32),
            pltpu.VMEM((TS, NT * 256), BF16),
            pltpu.VMEM((NT * 16, 128), I32),
            pltpu.VMEM((NT * 16, 128), F32),
            dma((3,)), dma((3,)), dma((2,)), dma((2,)), dma((2, 3)), dma((2, 3)), dma((2, 4, 3)), dma((2, 4, 3)),
            dma((4,)), dma((4,)), dma((2,)), dma((2,)), dma((2,)), regular, regular,
        ],
        compiler_params=pltpu.CompilerParams(collective_id=0, has_side_effects=True),
    )(*operands)


def shards(pair_map, visibilities, model_vis, flag_mask, gain_amp, gain_phase, row_index, cell_codes):
    grid, solved = whole(
        pair_map, visibilities, model_vis, flag_mask, row_index[0, 0], cell_codes.reshape(2, NT, 256),
        gain_amp.reshape(4, 128), gain_phase.reshape(4, 128),
    )
    return grid[None, None], solved


def solution(mesh):
    split = Mesh(mesh.devices.reshape(2, 4, 8, 2, 2), BLK + CHAN)
    placed = (
        P(BLK, None),
        P(None, BLK, CHAN, None),
        P(None, BLK, CHAN, None),
        P(BLK, CHAN, None),
        P(),
        P(),
        P(CHAN, BLK, None, None),
        P(None, CHAN, BLK, None, None),
    )
    return jax.shard_map(
        shards,
        mesh=split,
        in_specs=placed,
        out_specs=(P(CHAN, BLK, None, None, None), P()),
        check_vma=False,
    )
```

```python
import math

import jax
import jax.numpy as jnp
from jax import lax
from jax.experimental import pallas as pl
from jax.experimental.pallas import tpu as pltpu
from jax.sharding import Mesh
from jax.sharding import PartitionSpec as P

S = 512
BS = 32
NB = 16
ITERS = 3
TS = 128
NT = 64
CH = 16
F32 = jnp.float32
BF16 = jnp.bfloat16
I32 = jnp.int32
MESH = pl.DeviceIdType.MESH
BLK = ("blk_0", "blk_1", "blk_2")
CHAN = ("chan_0", "chan_1")
VM = pl.BlockSpec(memory_space=pltpu.VMEM)
SM = pl.BlockSpec(memory_space=pltpu.SMEM)


def iota(shape, axis):
    return lax.broadcasted_iota(I32, shape, axis)


def sums_and_tables(pm_ref, vis_ref, mod_ref, flag_ref, pq_ref, table_ref):
    for slot in range(2):
        first = pm_ref[slot, 0]
        second = pm_ref[slot, 1]
        same = (first == second).astype(F32)
        lane = iota((1, 128), 1)
        planes = [[], [], [], []]
        for tb in range(8):
            at = slice(tb * 128, tb * 128 + 128)
            base = lane + tb * 128
            diagonal = ((base >> 5) == (base & 31)).astype(F32)
            weight = flag_ref[slot, :, at].astype(F32) * (1.0 - same * diagonal)
            vr = vis_ref[0, slot, :, at].astype(F32) * weight
            vi = vis_ref[1, slot, :, at].astype(F32) * weight
            mr = mod_ref[0, slot, :, at].astype(F32) * weight
            mi = mod_ref[1, slot, :, at].astype(F32) * weight
            sums = (
                jnp.sum(vr * mr + vi * mi, axis=0, keepdims=True),
                jnp.sum(vi * mr - vr * mi, axis=0, keepdims=True),
                jnp.sum(mr * mr + mi * mi, axis=0, keepdims=True),
            )
            col = slice((tb % 2) * 128, (tb % 2) * 128 + 128)
            for q in range(3):
                row = slot * 3 + q
                pq_ref[tb // 2, row : row + 1, col] = sums[q]
            for plane, value in zip(planes, (vr, vi, mr, mi)):
                plane.append(value)
        for q in range(4):
            table = jnp.concatenate(planes[q], axis=0)
            table_ref[q * 128 : q * 128 + 128, slot * 128 : slot * 128 + 128] = table.T.astype(BF16)
        for quarter in range(4):
            col = slice(slot * 128, slot * 128 + 128)
            pq_ref[quarter, 6:7, col] = jnp.full((1, 128), first.astype(F32))
            pq_ref[quarter, 7:8, col] = jnp.full((1, 128), second.astype(F32))


def iota_table():
    return iota((256, 256), 0).astype(F32).astype(BF16)


def gather_tile(tile, index_ref, codes_ref, table_ref, iota_ref, rows_ref):
    index = index_ref[pl.ds(tile, 1), :]
    hi = ((index >> 14) << 7) | (((index >> 7) & 7) << 4) | ((index >> 10) & 15)
    high = jnp.broadcast_to(hi.astype(F32), (16, 256)).astype(BF16)
    one, zero = jnp.ones((16, 256), BF16), jnp.zeros((16, 256), BF16)
    onehot = jnp.concatenate(
        [jnp.where(iota_ref[k * 16 : k * 16 + 16, :] == high, one, zero) for k in range(16)], axis=0
    )
    lifted = jnp.dot(table_ref[...], onehot, preferred_element_type=F32)
    low_high = (index >> 3) & 15
    live = iota((8, 256), 0) == (index & 7)
    masks = [jnp.broadcast_to(low_high == k, (8, 256)) for k in range(16)]
    pieces = []
    for q in range(4):
        part = lifted[q * 128 : q * 128 + 8]
        for k in range(1, 16):
            part = jnp.where(masks[k], lifted[q * 128 + k * 8 : q * 128 + k * 8 + 8], part)
        value = jnp.sum(jnp.where(live, part, 0.0), axis=0, keepdims=True)
        pieces += [value[:, :128], value[:, 128:]]
    rows_ref[tile] = jnp.concatenate(pieces, axis=0).astype(BF16)


def write_ints(tile, index_ref, codes_ref, ints_ref):
    index = index_ref[pl.ds(tile, 1), :]
    both = codes_ref[0, pl.ds(tile, 1), :] | (codes_ref[1, pl.ds(tile, 1), :] << 16)
    place = (((index >> 14) & 1) << 10) | (index & 1023)
    ints_ref[tile] = jnp.concatenate([both[:, :128], both[:, 128:], place[:, :128], place[:, 128:]], axis=0)


def widen(all_ref, wide_ref, core):
    wide_ref[pl.ds(pl.multiple_of(core * 2048, 2048), 2048), :] = all_ref[core].astype(F32).reshape(2048, 128)


def wide_lines(wide_ref, core, xl, row):
    out = []
    for xh in range(2):
        for y in range(4):
            x = xh * 2 + xl
            place = core * 16 + (x * 4 + y) * (1 - core) + (y * 4 + x) * core
            out.append(wide_ref[pl.ds(place * 128 + row, 8, stride=16), :])
    return out


def turn(wide_ref, core, p_refs):
    for xl in range(2):
        for half in range(2):
            tb = (xl * 2 + core) * 2 + half
            for part in range(3):
                block = []
                for slot in range(2):
                    block += wide_lines(wide_ref, core, xl, half * 8 + slot * 3 + part)
                at = pl.ds(pl.multiple_of(tb * 128, 128), 128)
                p_refs[part][at, :] = jnp.concatenate(block, axis=0).T


def block_row(block):
    n = block.astype(I32)
    return ((n & 3) << 2) | (n >> 2)


def station_maps(wide_ref, core):
    found = []
    for side in range(2):
        for slot in range(2):
            found.append(block_row(jnp.concatenate(wide_lines(wide_ref, core, 0, slot * 8 + 6 + side), axis=0)))
    lane = iota((128, 128), 1)
    columns = [jnp.concatenate(found[:2], axis=0), jnp.concatenate(found[2:], axis=0)]
    onehot = jnp.concatenate([(c == lane).astype(F32) for c in columns], axis=0).astype(BF16)
    rows = [c.astype(F32).T[:32].astype(I32) for c in columns]
    lane = iota((NT, 128), 1)
    which = jnp.where(
        lane < 64, jnp.where(lane < 32, found[0], found[1]), jnp.where(lane < 96, found[2], found[3])
    )
    return onehot, rows, which


def start_gains(amp_ref, phase_ref):
    amp, phase = amp_ref[...], phase_ref[...]
    out = []
    for value in (amp * jnp.cos(phase), amp * jnp.sin(phase)):
        stacked = jnp.concatenate([value[:, a * 32 : a * 32 + 32] for a in range(4)], axis=0)
        stacked = jnp.concatenate([stacked, jnp.zeros((112, 32), F32)], axis=0)
        out.append(stacked.T)
    return out


def station_sums(terms, onehot):
    high = terms.astype(BF16)
    rest = terms - high.astype(F32)
    middle = rest.astype(BF16)
    low = (rest - middle.astype(F32)).astype(BF16)
    sums = jnp.dot(jnp.concatenate([high, middle, low], axis=0), onehot, preferred_element_type=F32)
    return sums[:96] + (sums[96:192] + sums[192:])


def solve(gr, gi, onehot, rows, p_refs):
    def spread(g, which):
        return jnp.take_along_axis(g, rows[which], axis=1)

    pr_ref, pi_ref, q_ref = p_refs
    for sweep in range(ITERS):
        ar, ai, br, bi = spread(gr, 0), spread(gi, 0), spread(gr, 1), spread(gi, 1)
        a2 = ar * ar + ai * ai
        b2 = br * br + bi * bi
        zero = jnp.zeros((32, 128), F32)
        first = [zero, zero, zero]
        second = [zero, zero, zero]
        for i in range(32):
            pr = pr_ref[i * 32 : i * 32 + 32, :]
            pi = pi_ref[i * 32 : i * 32 + 32, :]
            q = q_ref[i * 32 : i * 32 + 32, :]
            xr, xi, x2 = ar[i : i + 1], ai[i : i + 1], a2[i : i + 1]
            second[0] = second[0] + (pr * xr + pi * xi)
            second[1] = second[1] + (pr * xi - pi * xr)
            second[2] = second[2] + q * x2
        for j in range(32):
            at = pl.ds(j, 32, stride=32)
            pr, pi, q = pr_ref[at, :], pi_ref[at, :], q_ref[at, :]
            xr, xi, x2 = br[j : j + 1], bi[j : j + 1], b2[j : j + 1]
            first[0] = first[0] + (pr * xr - pi * xi)
            first[1] = first[1] + (pr * xi + pi * xr)
            first[2] = first[2] + q * x2
        terms = jnp.concatenate([jnp.concatenate(first, axis=0), jnp.concatenate(second, axis=0)], axis=1)
        total = station_sums(terms, onehot)
        denominator = jnp.where(iota((32, 128), 1) < NB, total[64:96], 1.0)
        ur = total[0:32] / denominator
        ui = total[32:64] / denominator
        if sweep % 2 == 1:
            gr, gi = 0.5 * (ur + gr), 0.5 * (ui + gi)
        else:
            gr, gi = ur, ui
    return gr, gi


def residual_rows(gr, gi, which, lines_ref, ints_ref, res_ref):
    turned_r = gr.T[:NB, :]
    turned_i = gi.T[:NB, :]
    turned_r = jnp.concatenate([turned_r] * 4, axis=1)
    turned_i = jnp.concatenate([turned_i] * 4, axis=1)

    table_r = jnp.zeros((NT, 128), F32)
    table_i = jnp.zeros((NT, 128), F32)
    for n in range(NB):
        hit = which == n
        table_r = jnp.where(hit, turned_r[n : n + 1], table_r)
        table_i = jnp.where(hit, turned_i[n : n + 1], table_i)
    for half in range(2):
        place = ints_ref[:, 2 + half, :]
        slot = (place >> 10) * 32
        at_a = slot + ((place >> 5) & 31)
        at_b = slot + (place & 31) + 64
        ar = jnp.take_along_axis(table_r, at_a, axis=1)
        ai = jnp.take_along_axis(table_i, at_a, axis=1)
        br = jnp.take_along_axis(table_r, at_b, axis=1)
        bi = jnp.take_along_axis(table_i, at_b, axis=1)
        vr, vi, mr, mi = (lines_ref[pl.ds(q * 2 + half, NT, stride=8), :] for q in range(4))
        twisted_r = mr * br + mi * bi
        twisted_i = mi * br - mr * bi
        res_ref[0, half] = (vr - (ar * twisted_r - ai * twisted_i)).astype(BF16).astype(F32)
        res_ref[1, half] = (vi - (ar * twisted_i + ai * twisted_r)).astype(BF16).astype(F32)


def doubled(block):
    return jnp.concatenate([block, block - 1.0], axis=0).astype(BF16)


def spread_out(place, values):
    zero = jnp.zeros((16, 128), BF16)
    hits = [place == jnp.full((16, 128), 2.0 * k, BF16) for k in range(8)]
    out = []
    for value in values:
        both = jnp.concatenate([value, value], axis=0).astype(BF16)
        out += [jnp.where(hit, both, zero) for hit in hits]
    return jnp.concatenate(out, axis=0)


def window(code):
    shifted = iota((8, 128), 0) * 8 - code
    block = (32 - shifted) >> 6
    distance = block * 64 + shifted
    angle = distance.astype(F32) * (math.pi / 64)
    z = angle * angle
    cos = 1.0 / math.factorial(14)
    for k in range(6, -1, -1):
        cos = 1.0 / math.factorial(2 * k) - z * cos
    value = jnp.where(jnp.abs(distance) < 32, cos * cos, 0.0).astype(BF16).astype(F32)
    return block.astype(F32), value


NEAR = (1, 3, 2)
SLOT = (0, 1, 3, 5, 7, 6, 4, 2)
GROUPS = ((0, 5), (5, 3))
CUT = (16, 28, 40)


def kernel(
    pm_ref, vis_ref, mod_ref, flag_ref, index_ref, codes_ref, amp_ref, phase_ref,
    grid_ref, solved_ref,
    table_ref, iota_ref, pq_ref, rows_ref, ints_ref, part, all_ref, got_rows, got_ints,
    wide_ref, pr_ref, pi_ref, q_ref, lines_ref, res_ref, left_ref, vblock_ref, vvalue_ref,
    sum_send, sum_recv, line_send, line_recv, in_send, in_recv, out_send, out_recv,
    core_send, core_recv, a2a_send, a2a_recv, own_sem, plane_sem, far_sem,
):
    xh, y, z = lax.axis_index("blk_0"), lax.axis_index("blk_1"), lax.axis_index("blk_2")
    xl, core = lax.axis_index("chan_0"), lax.axis_index("chan_1")
    me = xh * 4 + y
    x = xh * 2 + xl
    quarter = xl * 2 + core
    inner = y * (1 - core) + x * core
    outer = x * (1 - core) + y * core

    def chan_id(step):
        c = lax.rem(quarter + step, 4)
        return c, {"chan_0": c // 2, "chan_1": lax.rem(c, 2)}

    def line_id(step):
        return {"blk_2": lax.rem(z + step, 8)}

    def y_id(step):
        return {"blk_1": lax.rem(y + step, 4)}

    def x_id(step):
        return {"blk_0": lax.rem(x + step, 4) // 2, "chan_0": lax.rem(x + step, 2)}

    def plane_id(in_step, out_step):
        i, o = lax.rem(inner + in_step, 4), lax.rem(outer + out_step, 4)
        py = i * (1 - core) + o * core
        px = o * (1 - core) + i * core
        return {"blk_0": px // 2, "chan_0": lax.rem(px, 2), "blk_1": py}

    def signal(sem, device):
        pl.semaphore_signal(sem, inc=1, device_id=device, device_id_type=MESH)

    barrier = pltpu.get_barrier_semaphore()
    for step in range(1, 4):
        signal(barrier, chan_id(step)[1])
        signal(barrier, x_id(step))
        signal(barrier, y_id(step))
    for step in range(1, 8):
        signal(barrier, line_id(step))

    def remote(src, dst, send, recv, device):
        return pltpu.make_async_remote_copy(
            src_ref=src, dst_ref=dst, send_sem=send, recv_sem=recv, device_id=device, device_id_type=MESH
        )

    def gather(first, last):
        def step(group, carry):
            for member in range(4):
                gather_tile(group * 4 + member, index_ref, codes_ref, table_ref, iota_ref, rows_ref)
            return carry

        lax.fori_loop(first // 4, last // 4, step, 0)

    def to_owners(src, dst, k):
        for away in range(8):
            tz = lax.rem(z + away, 8)
            slot = SLOT[(8 - away) % 8]

            def step(n, carry):
                line = lax.rem(me + n, 8)
                device = {"blk_0": line // 4, "blk_1": lax.rem(line, 4), "blk_2": tz}
                remote(src.at[line * 8 + tz], dst.at[me * 8 + slot], a2a_send.at[k], a2a_recv.at[k], device).start()
                return carry

            lax.fori_loop(1 if away == 0 else 0, 8, step, 0)
        keep = pltpu.make_async_copy(src.at[me * 8 + z], dst.at[me * 8], own_sem.at[k])
        keep.start()
        return keep

    def owners_done(buf, k, keep):
        span = buf.at[pl.ds(0, NT - 1)]
        remote(span, span, a2a_send.at[k], a2a_recv.at[k], {"chan_1": 1 - core}).wait()
        keep.wait()

    sums_and_tables(pm_ref, vis_ref, mod_ref, flag_ref, pq_ref, table_ref)
    pl.semaphore_wait(barrier, 16)
    for step in range(1, 4):
        signal(plane_sem, y_id(step))

    def piece(step):
        c, device = chan_id(step)
        return remote(pq_ref.at[c], part.at[step - 1], sum_send.at[step - 1], sum_recv.at[step - 1], device)

    for step in range(1, 4):
        piece(step).start()
    iota_ref[...] = iota_table()

    def ints_step(group, carry):
        for member in range(4):
            write_ints(group * 4 + member, index_ref, codes_ref, ints_ref)
        return carry

    lax.fori_loop(0, NT // 4, ints_step, 0)
    gather(0, CUT[0])
    total = pq_ref[quarter]
    for step in range(1, 4):
        piece(step).wait_recv()
        total = total + part[step - 1]
    total = jnp.concatenate([total[:6], pq_ref[0, 6:8, :]], axis=0)
    all_ref[core, outer, inner, 0] = jnp.concatenate([total[:, :128], total[:, 128:]], axis=0).astype(BF16)

    mine = all_ref.at[core, outer, inner, 0]

    def along(step):
        slot = SLOT[(8 - step) % 8]
        k = 0 if slot < 5 else 1
        return remote(mine, all_ref.at[core, outer, inner, slot], line_send.at[k], line_recv.at[k], line_id(step))

    for step in (1, 7, 2, 6, 3, 5, 4):
        along(step).start()
    pl.semaphore_wait(plane_sem, 3)
    signal(far_sem, {"blk_0": 1 - xh})
    pl.semaphore_wait(far_sem, 1)
    keep_ints = to_owners(ints_ref, got_ints, 1)
    gather(CUT[0], CUT[1])

    def line(k):
        count = (4, 3)[k]
        span = all_ref.at[core, outer, inner, pl.ds(0, count)]
        return remote(span, span, line_send.at[k], line_recv.at[k], line_id(1))

    def block(back, k):
        return all_ref.at[core, outer, lax.rem(inner + 4 - back, 4), pl.ds(*GROUPS[k])]

    def inward(step, k):
        src = block(0, k)
        return remote(src, src, in_send.at[k, step - 1], in_recv.at[k, step - 1], plane_id(step, 0))

    def outward(back, step, k):
        src = block(back, k)
        return remote(src, src, out_send.at[k, back, step - 1], out_recv.at[k, back, step - 1], plane_id(0, step))

    for k in range(2):
        line(k).wait_recv()
        for step in NEAR:
            inward(step, k).start()
        for step in NEAR:
            outward(0, step, k).start()
        if k == 0:
            gather(CUT[1], CUT[2])
    gather(CUT[2], NT)
    for k in range(2):
        for back in NEAR:
            inward(back, k).wait_recv()
            for step in NEAR:
                outward(back, step, k).start()
    keep_rows = to_owners(rows_ref, got_rows, 0)

    owners_done(got_ints, 1, keep_ints)

    def windows(group, carry):
        for member in range(4):
            s = group * 4 + member
            for half in range(2):
                both = got_ints[s, half : half + 1, :]
                ublock, uvalue = window(both & 65535)
                vblock, vvalue = window(both >> 16)
                at = pl.ds(pl.multiple_of((s * 2 + half) * 8, 8), 8)
                vblock_ref[at, :] = vblock
                vvalue_ref[at, :] = vvalue
                left_ref[:, pl.ds(pl.multiple_of((s * 2 + half) * 128, 128), 128)] = spread_out(doubled(ublock), [uvalue])
        return carry

    lax.fori_loop(0, NT // 4, windows, 0)
    gr, gi = start_gains(amp_ref, phase_ref)

    def across(back):
        src = all_ref.at[core, lax.rem(outer + 4 - back, 4)]
        return remote(src, src, core_send.at[back], core_recv.at[back], {"chan_1": 1 - core})

    across(0).start()
    for step in NEAR:
        for k in range(2):
            for back in (0,) + NEAR:
                outward(back, step, k).wait_recv()
        across(step).start()

    p_refs = (pr_ref, pi_ref, q_ref)
    widen(all_ref, wide_ref, core)
    turn(wide_ref, core, p_refs)
    onehot, rows, which = station_maps(wide_ref, core)
    for step in range(4):
        across(step).wait_recv()
    widen(all_ref, wide_ref, 1 - core)
    turn(wide_ref, 1 - core, p_refs)
    gr, gi = solve(gr, gi, onehot, rows, p_refs)
    for part_at, g in enumerate((gr, gi)):
        turned = g.T
        at = [(n % 4) * 4 + n // 4 for n in range(NB)]
        solved_ref[part_at : part_at + 1, :] = jnp.concatenate([turned[n : n + 1, :] for n in at], axis=1)

    owners_done(got_rows, 0, keep_rows)
    lines_ref[...] = got_rows[...].astype(F32).reshape(512, 128)
    residual_rows(gr, gi, which, lines_ref, got_ints, res_ref)

    def half_tile(s, half):
        at = pl.ds(pl.multiple_of((s * 2 + half) * 8, 8), 8)
        place, vvalue = doubled(vblock_ref[at, :]), vvalue_ref[at, :]
        values = [vvalue * res_ref[p, half, pl.ds(s, 1), :] for p in range(2)]
        return spread_out(place, values)

    def grid_step(step, acc):
        for piece_at in range(4):
            group = step * 4 + piece_at
            members = [half_tile(group * 8 + member, half) for member in range(8) for half in range(2)]
            left = left_ref[:, pl.ds(pl.multiple_of(group * 2048, 2048), 2048)]
            right = jnp.concatenate(members, axis=1)
            acc = acc + lax.dot_general(right, left, (((1,), (1,)), ((), ())), preferred_element_type=F32)
        return acc

    acc = lax.fori_loop(0, NT // 32, grid_step, jnp.zeros((2 * TS, TS), F32))
    grid_ref[0] = acc[:TS].T
    grid_ref[1] = acc[TS:].T

    for k in range(2):
        line(k).wait_send()
        for step in range(1, 4):
            inward(step, k).wait_send()
            for back in range(4):
                outward(back, step, k).wait_send()
    for step in range(1, 4):
        piece(step).wait_send()
    for step in range(4):
        across(step).wait_send()


def whole(*operands):
    dma, regular = pltpu.SemaphoreType.DMA, pltpu.SemaphoreType.REGULAR
    return pl.pallas_call(
        kernel,
        name="whole",
        out_shape=(
            jax.ShapeDtypeStruct((2, TS, TS), F32),
            jax.ShapeDtypeStruct((2, S), F32),
        ),
        in_specs=[SM] + [VM] * 7,
        out_specs=(VM, VM),
        scratch_shapes=[
            pltpu.VMEM((512, 256), BF16),
            pltpu.VMEM((256, 256), BF16),
            pltpu.VMEM((4, 8, 256), F32),
            pltpu.VMEM((NT, 8, 128), BF16),
            pltpu.VMEM((NT, 4, 128), I32),
            pltpu.VMEM((3, 8, 256), F32),
            pltpu.VMEM((2, 4, 4, 8, 16, 128), BF16),
            pltpu.VMEM((NT, 8, 128), BF16),
            pltpu.VMEM((NT, 4, 128), I32),
            pltpu.VMEM((4096, 128), F32),
            pltpu.VMEM((1024, 128), F32),
            pltpu.VMEM((1024, 128), F32),
            pltpu.VMEM((1024, 128), F32),
            pltpu.VMEM((512, 128), F32),
            pltpu.VMEM((2, 2, NT, 128), F32),
            pltpu.VMEM((TS, NT * 256), BF16),
            pltpu.VMEM((NT * 16, 128), F32),
            pltpu.VMEM((NT * 16, 128), F32),
            dma((3,)), dma((3,)), dma((2,)), dma((2,)), dma((2, 3)), dma((2, 3)), dma((2, 4, 3)), dma((2, 4, 3)),
            dma((4,)), dma((4,)), dma((2,)), dma((2,)), dma((2,)), regular, regular,
        ],
        compiler_params=pltpu.CompilerParams(collective_id=0, has_side_effects=True),
    )(*operands)


def shards(pair_map, visibilities, model_vis, flag_mask, gain_amp, gain_phase, row_index, cell_codes):
    grid, solved = whole(
        pair_map, visibilities, model_vis, flag_mask, row_index[0, 0], cell_codes.reshape(2, NT, 256),
        gain_amp.reshape(4, 128), gain_phase.reshape(4, 128),
    )
    return grid[None, None], solved


def solution(mesh):
    split = Mesh(mesh.devices.reshape(2, 4, 8, 2, 2), BLK + CHAN)
    placed = (
        P(BLK, None),
        P(None, BLK, CHAN, None),
        P(None, BLK, CHAN, None),
        P(BLK, CHAN, None),
        P(),
        P(),
        P(CHAN, BLK, None, None),
        P(None, CHAN, BLK, None, None),
    )
    return jax.shard_map(
        shards,
        mesh=split,
        in_specs=placed,
        out_specs=(P(CHAN, BLK, None, None, None), P()),
        check_vma=False,
    )
```

```python
import math

import jax
import jax.numpy as jnp
from jax import lax
from jax.experimental import pallas as pl
from jax.experimental.pallas import tpu as pltpu
from jax.sharding import Mesh
from jax.sharding import PartitionSpec as P

S = 512
BS = 32
NB = 16
ITERS = 3
TS = 128
NT = 64
CH = 16
F32 = jnp.float32
BF16 = jnp.bfloat16
I32 = jnp.int32
MESH = pl.DeviceIdType.MESH
BLK = ("blk_0", "blk_1", "blk_2")
CHAN = ("chan_0", "chan_1")
VM = pl.BlockSpec(memory_space=pltpu.VMEM)
SM = pl.BlockSpec(memory_space=pltpu.SMEM)


def iota(shape, axis):
    return lax.broadcasted_iota(I32, shape, axis)


def weighted(pm_ref, vis_ref, mod_ref, flag_ref, slot, tb):
    same = (pm_ref[slot, 0] == pm_ref[slot, 1]).astype(F32)
    at = slice(tb * 128, tb * 128 + 128)
    base = iota((1, 128), 1) + tb * 128
    diagonal = ((base >> 5) == (base & 31)).astype(F32)
    weight = flag_ref[slot, :, at].astype(F32) * (1.0 - same * diagonal)
    return [ref[c, slot, :, at].astype(F32) * weight for ref in (vis_ref, mod_ref) for c in range(2)]


def channel_sums(pm_ref, vis_ref, mod_ref, flag_ref, pq_ref):
    for slot in range(2):
        for tb in range(8):
            vr, vi, mr, mi = weighted(pm_ref, vis_ref, mod_ref, flag_ref, slot, tb)
            sums = (
                jnp.sum(vr * mr + vi * mi, axis=0, keepdims=True),
                jnp.sum(vi * mr - vr * mi, axis=0, keepdims=True),
                jnp.sum(mr * mr + mi * mi, axis=0, keepdims=True),
            )
            col = slice((tb % 2) * 128, (tb % 2) * 128 + 128)
            for q in range(3):
                row = slot * 3 + q
                pq_ref[tb // 2, row : row + 1, col] = sums[q]
        for quarter in range(4):
            col = slice(slot * 128, slot * 128 + 128)
            pq_ref[quarter, 6:7, col] = jnp.full((1, 128), pm_ref[slot, 0].astype(F32))
            pq_ref[quarter, 7:8, col] = jnp.full((1, 128), pm_ref[slot, 1].astype(F32))


def gather_tables(pm_ref, vis_ref, mod_ref, flag_ref, table_ref):
    for slot in range(2):
        planes = [weighted(pm_ref, vis_ref, mod_ref, flag_ref, slot, tb) for tb in range(8)]
        for q in range(4):
            table = jnp.concatenate([plane[q] for plane in planes], axis=0)
            table_ref[q * 128 : q * 128 + 128, slot * 128 : slot * 128 + 128] = table.T.astype(BF16)


def iota_table():
    return iota((256, 256), 0).astype(F32).astype(BF16)


def gather_tile(tile, index_ref, codes_ref, table_ref, iota_ref, rows_ref):
    index = index_ref[pl.ds(tile, 1), :]
    hi = ((index >> 14) << 7) | (((index >> 7) & 7) << 4) | ((index >> 10) & 15)
    high = jnp.broadcast_to(hi.astype(F32), (16, 256)).astype(BF16)
    one, zero = jnp.ones((16, 256), BF16), jnp.zeros((16, 256), BF16)
    onehot = jnp.concatenate(
        [jnp.where(iota_ref[k * 16 : k * 16 + 16, :] == high, one, zero) for k in range(16)], axis=0
    )
    lifted = jnp.dot(table_ref[...], onehot, preferred_element_type=F32)
    low_high = (index >> 3) & 15
    live = iota((8, 256), 0) == (index & 7)
    masks = [jnp.broadcast_to(low_high == k, (8, 256)) for k in range(16)]
    pieces = []
    for q in range(4):
        part = lifted[q * 128 : q * 128 + 8]
        for k in range(1, 16):
            part = jnp.where(masks[k], lifted[q * 128 + k * 8 : q * 128 + k * 8 + 8], part)
        value = jnp.sum(jnp.where(live, part, 0.0), axis=0, keepdims=True)
        pieces += [value[:, :128], value[:, 128:]]
    rows_ref[tile] = jnp.concatenate(pieces, axis=0).astype(BF16)


def write_ints(tile, index_ref, codes_ref, ints_ref):
    index = index_ref[pl.ds(tile, 1), :]
    both = codes_ref[0, pl.ds(tile, 1), :] | (codes_ref[1, pl.ds(tile, 1), :] << 16)
    place = (((index >> 14) & 1) << 10) | (index & 1023)
    ints_ref[tile] = jnp.concatenate([both[:, :128], both[:, 128:], place[:, :128], place[:, 128:]], axis=0)


def widen(all_ref, wide_ref, core):
    wide_ref[pl.ds(pl.multiple_of(core * 2048, 2048), 2048), :] = all_ref[core].astype(F32).reshape(2048, 128)


def wide_lines(wide_ref, core, xl, row):
    out = []
    for xh in range(2):
        for y in range(4):
            x = xh * 2 + xl
            place = core * 16 + (x * 4 + y) * (1 - core) + (y * 4 + x) * core
            out.append(wide_ref[pl.ds(place * 128 + row, 8, stride=16), :])
    return out


def turn(wide_ref, core, p_refs):
    for xl in range(2):
        for half in range(2):
            tb = (xl * 2 + core) * 2 + half
            for part in range(3):
                block = []
                for slot in range(2):
                    block += wide_lines(wide_ref, core, xl, half * 8 + slot * 3 + part)
                at = pl.ds(pl.multiple_of(tb * 128, 128), 128)
                p_refs[part][at, :] = jnp.concatenate(block, axis=0).T


def block_row(block):
    n = block.astype(I32)
    return ((n & 3) << 2) | (n >> 2)


def station_maps(wide_ref, core):
    found = []
    for side in range(2):
        for slot in range(2):
            found.append(block_row(jnp.concatenate(wide_lines(wide_ref, core, 0, slot * 8 + 6 + side), axis=0)))
    lane = iota((128, 128), 1)
    columns = [jnp.concatenate(found[:2], axis=0), jnp.concatenate(found[2:], axis=0)]
    onehot = jnp.concatenate([(c == lane).astype(F32) for c in columns], axis=0).astype(BF16)
    rows = [c.astype(F32).T[:32].astype(I32) for c in columns]
    lane = iota((NT, 128), 1)
    which = jnp.where(
        lane < 64, jnp.where(lane < 32, found[0], found[1]), jnp.where(lane < 96, found[2], found[3])
    )
    return onehot, rows, which


def start_gains(amp_ref, phase_ref):
    amp, phase = amp_ref[...], phase_ref[...]
    out = []
    for value in (amp * jnp.cos(phase), amp * jnp.sin(phase)):
        stacked = jnp.concatenate([value[:, a * 32 : a * 32 + 32] for a in range(4)], axis=0)
        stacked = jnp.concatenate([stacked, jnp.zeros((112, 32), F32)], axis=0)
        out.append(stacked.T)
    return out


def station_sums(terms, onehot):
    high = terms.astype(BF16)
    rest = terms - high.astype(F32)
    middle = rest.astype(BF16)
    low = (rest - middle.astype(F32)).astype(BF16)
    sums = jnp.dot(jnp.concatenate([high, middle, low], axis=0), onehot, preferred_element_type=F32)
    return sums[:96] + (sums[96:192] + sums[192:])


def solve(gr, gi, onehot, rows, p_refs):
    def spread(g, which):
        return jnp.take_along_axis(g, rows[which], axis=1)

    pr_ref, pi_ref, q_ref = p_refs
    for sweep in range(ITERS):
        ar, ai, br, bi = spread(gr, 0), spread(gi, 0), spread(gr, 1), spread(gi, 1)
        a2 = ar * ar + ai * ai
        b2 = br * br + bi * bi
        zero = jnp.zeros((32, 128), F32)
        first = [zero, zero, zero]
        second = [zero, zero, zero]
        for i in range(32):
            pr = pr_ref[i * 32 : i * 32 + 32, :]
            pi = pi_ref[i * 32 : i * 32 + 32, :]
            q = q_ref[i * 32 : i * 32 + 32, :]
            xr, xi, x2 = ar[i : i + 1], ai[i : i + 1], a2[i : i + 1]
            second[0] = second[0] + (pr * xr + pi * xi)
            second[1] = second[1] + (pr * xi - pi * xr)
            second[2] = second[2] + q * x2
        for j in range(32):
            at = pl.ds(j, 32, stride=32)
            pr, pi, q = pr_ref[at, :], pi_ref[at, :], q_ref[at, :]
            xr, xi, x2 = br[j : j + 1], bi[j : j + 1], b2[j : j + 1]
            first[0] = first[0] + (pr * xr - pi * xi)
            first[1] = first[1] + (pr * xi + pi * xr)
            first[2] = first[2] + q * x2
        terms = jnp.concatenate([jnp.concatenate(first, axis=0), jnp.concatenate(second, axis=0)], axis=1)
        total = station_sums(terms, onehot)
        denominator = jnp.where(iota((32, 128), 1) < NB, total[64:96], 1.0)
        ur = total[0:32] / denominator
        ui = total[32:64] / denominator
        if sweep % 2 == 1:
            gr, gi = 0.5 * (ur + gr), 0.5 * (ui + gi)
        else:
            gr, gi = ur, ui
    return gr, gi


def residual_rows(gr, gi, which, lines_ref, ints_ref, res_ref):
    turned_r = gr.T[:NB, :]
    turned_i = gi.T[:NB, :]
    turned_r = jnp.concatenate([turned_r] * 4, axis=1)
    turned_i = jnp.concatenate([turned_i] * 4, axis=1)

    table_r = jnp.zeros((NT, 128), F32)
    table_i = jnp.zeros((NT, 128), F32)
    for n in range(NB):
        hit = which == n
        table_r = jnp.where(hit, turned_r[n : n + 1], table_r)
        table_i = jnp.where(hit, turned_i[n : n + 1], table_i)
    for half in range(2):
        place = ints_ref[:, 2 + half, :]
        slot = (place >> 10) * 32
        at_a = slot + ((place >> 5) & 31)
        at_b = slot + (place & 31) + 64
        ar = jnp.take_along_axis(table_r, at_a, axis=1)
        ai = jnp.take_along_axis(table_i, at_a, axis=1)
        br = jnp.take_along_axis(table_r, at_b, axis=1)
        bi = jnp.take_along_axis(table_i, at_b, axis=1)
        vr, vi, mr, mi = (lines_ref[pl.ds(q * 2 + half, NT, stride=8), :] for q in range(4))
        twisted_r = mr * br + mi * bi
        twisted_i = mi * br - mr * bi
        res_ref[0, half] = (vr - (ar * twisted_r - ai * twisted_i)).astype(BF16).astype(F32)
        res_ref[1, half] = (vi - (ar * twisted_i + ai * twisted_r)).astype(BF16).astype(F32)


def doubled(block):
    return jnp.concatenate([block, block - 1.0], axis=0).astype(BF16)


def spread_out(place, values):
    zero = jnp.zeros((16, 128), BF16)
    hits = [place == jnp.full((16, 128), 2.0 * k, BF16) for k in range(8)]
    out = []
    for value in values:
        both = jnp.concatenate([value, value], axis=0).astype(BF16)
        out += [jnp.where(hit, both, zero) for hit in hits]
    return jnp.concatenate(out, axis=0)


def window(code):
    shifted = iota((8, 128), 0) * 8 - code
    block = (32 - shifted) >> 6
    distance = block * 64 + shifted
    angle = distance.astype(F32) * (math.pi / 64)
    z = angle * angle
    cos = 1.0 / math.factorial(14)
    for k in range(6, -1, -1):
        cos = 1.0 / math.factorial(2 * k) - z * cos
    value = jnp.where(jnp.abs(distance) < 32, cos * cos, 0.0).astype(BF16).astype(F32)
    return block.astype(F32), value


NEAR = (1, 3, 2)
SLOT = (0, 1, 3, 5, 7, 6, 4, 2)
GROUPS = ((0, 5), (5, 3))
CUT = (16, 28, 40)


def kernel(
    pm_ref, vis_ref, mod_ref, flag_ref, index_ref, codes_ref, amp_ref, phase_ref,
    grid_ref, solved_ref,
    table_ref, iota_ref, pq_ref, rows_ref, ints_ref, part, all_ref, got_rows, got_ints,
    wide_ref, pr_ref, pi_ref, q_ref, lines_ref, res_ref, left_ref, vblock_ref, vvalue_ref,
    sum_send, sum_recv, line_send, line_recv, in_send, in_recv, out_send, out_recv,
    core_send, core_recv, a2a_send, a2a_recv, own_sem, plane_sem, far_sem,
):
    xh, y, z = lax.axis_index("blk_0"), lax.axis_index("blk_1"), lax.axis_index("blk_2")
    xl, core = lax.axis_index("chan_0"), lax.axis_index("chan_1")
    me = xh * 4 + y
    x = xh * 2 + xl
    quarter = xl * 2 + core
    inner = y * (1 - core) + x * core
    outer = x * (1 - core) + y * core

    def chan_id(step):
        c = lax.rem(quarter + step, 4)
        return c, {"chan_0": c // 2, "chan_1": lax.rem(c, 2)}

    def line_id(step):
        return {"blk_2": lax.rem(z + step, 8)}

    def y_id(step):
        return {"blk_1": lax.rem(y + step, 4)}

    def x_id(step):
        return {"blk_0": lax.rem(x + step, 4) // 2, "chan_0": lax.rem(x + step, 2)}

    def plane_id(in_step, out_step):
        i, o = lax.rem(inner + in_step, 4), lax.rem(outer + out_step, 4)
        py = i * (1 - core) + o * core
        px = o * (1 - core) + i * core
        return {"blk_0": px // 2, "chan_0": lax.rem(px, 2), "blk_1": py}

    def signal(sem, device):
        pl.semaphore_signal(sem, inc=1, device_id=device, device_id_type=MESH)

    barrier = pltpu.get_barrier_semaphore()
    for step in range(1, 4):
        signal(barrier, chan_id(step)[1])
        signal(barrier, x_id(step))
        signal(barrier, y_id(step))
    for step in range(1, 8):
        signal(barrier, line_id(step))

    def remote(src, dst, send, recv, device):
        return pltpu.make_async_remote_copy(
            src_ref=src, dst_ref=dst, send_sem=send, recv_sem=recv, device_id=device, device_id_type=MESH
        )

    def gather(first, last):
        def step(group, carry):
            for member in range(4):
                gather_tile(group * 4 + member, index_ref, codes_ref, table_ref, iota_ref, rows_ref)
            return carry

        lax.fori_loop(first // 4, last // 4, step, 0)

    def to_owners(src, dst, k):
        for away in range(8):
            tz = lax.rem(z + away, 8)
            slot = SLOT[(8 - away) % 8]

            def step(n, carry):
                line = lax.rem(me + n, 8)
                device = {"blk_0": line // 4, "blk_1": lax.rem(line, 4), "blk_2": tz}
                remote(src.at[line * 8 + tz], dst.at[me * 8 + slot], a2a_send.at[k], a2a_recv.at[k], device).start()
                return carry

            lax.fori_loop(1 if away == 0 else 0, 8, step, 0)
        keep = pltpu.make_async_copy(src.at[me * 8 + z], dst.at[me * 8], own_sem.at[k])
        keep.start()
        return keep

    def owners_done(buf, k, keep):
        span = buf.at[pl.ds(0, NT - 1)]
        remote(span, span, a2a_send.at[k], a2a_recv.at[k], {"chan_1": 1 - core}).wait()
        keep.wait()

    channel_sums(pm_ref, vis_ref, mod_ref, flag_ref, pq_ref)
    pl.semaphore_wait(barrier, 16)
    for step in range(1, 4):
        signal(plane_sem, y_id(step))

    def piece(step):
        c, device = chan_id(step)
        return remote(pq_ref.at[c], part.at[step - 1], sum_send.at[step - 1], sum_recv.at[step - 1], device)

    for step in range(1, 4):
        piece(step).start()
    gather_tables(pm_ref, vis_ref, mod_ref, flag_ref, table_ref)
    iota_ref[...] = iota_table()

    def ints_step(group, carry):
        for member in range(4):
            write_ints(group * 4 + member, index_ref, codes_ref, ints_ref)
        return carry

    lax.fori_loop(0, NT // 4, ints_step, 0)
    gather(0, CUT[0])
    total = pq_ref[quarter]
    for step in range(1, 4):
        piece(step).wait_recv()
        total = total + part[step - 1]
    total = jnp.concatenate([total[:6], pq_ref[0, 6:8, :]], axis=0)
    all_ref[core, outer, inner, 0] = jnp.concatenate([total[:, :128], total[:, 128:]], axis=0).astype(BF16)

    mine = all_ref.at[core, outer, inner, 0]

    def along(step):
        slot = SLOT[(8 - step) % 8]
        k = 0 if slot < 5 else 1
        return remote(mine, all_ref.at[core, outer, inner, slot], line_send.at[k], line_recv.at[k], line_id(step))

    for step in (1, 7, 2, 6, 3, 5, 4):
        along(step).start()
    pl.semaphore_wait(plane_sem, 3)
    signal(far_sem, {"blk_0": 1 - xh})
    gather(CUT[0], CUT[1])
    pl.semaphore_wait(far_sem, 1)
    keep_ints = to_owners(ints_ref, got_ints, 1)

    def line(k):
        count = (4, 3)[k]
        span = all_ref.at[core, outer, inner, pl.ds(0, count)]
        return remote(span, span, line_send.at[k], line_recv.at[k], line_id(1))

    def block(back, k):
        return all_ref.at[core, outer, lax.rem(inner + 4 - back, 4), pl.ds(*GROUPS[k])]

    def inward(step, k):
        src = block(0, k)
        return remote(src, src, in_send.at[k, step - 1], in_recv.at[k, step - 1], plane_id(step, 0))

    def outward(back, step, k):
        src = block(back, k)
        return remote(src, src, out_send.at[k, back, step - 1], out_recv.at[k, back, step - 1], plane_id(0, step))

    for k in range(2):
        line(k).wait_recv()
        for step in NEAR:
            inward(step, k).start()
        for step in NEAR:
            outward(0, step, k).start()
        if k == 0:
            gather(CUT[1], CUT[2])
    gather(CUT[2], NT)
    for k in range(2):
        for back in NEAR:
            inward(back, k).wait_recv()
            for step in NEAR:
                outward(back, step, k).start()
    keep_rows = to_owners(rows_ref, got_rows, 0)

    owners_done(got_ints, 1, keep_ints)

    def windows(group, carry):
        for member in range(4):
            s = group * 4 + member
            for half in range(2):
                both = got_ints[s, half : half + 1, :]
                ublock, uvalue = window(both & 65535)
                vblock, vvalue = window(both >> 16)
                at = pl.ds(pl.multiple_of((s * 2 + half) * 8, 8), 8)
                vblock_ref[at, :] = vblock
                vvalue_ref[at, :] = vvalue
                left_ref[:, pl.ds(pl.multiple_of((s * 2 + half) * 128, 128), 128)] = spread_out(doubled(ublock), [uvalue])
        return carry

    lax.fori_loop(0, NT // 4, windows, 0)
    gr, gi = start_gains(amp_ref, phase_ref)

    def across(back):
        src = all_ref.at[core, lax.rem(outer + 4 - back, 4)]
        return remote(src, src, core_send.at[back], core_recv.at[back], {"chan_1": 1 - core})

    across(0).start()
    for step in NEAR:
        for k in range(2):
            for back in (0,) + NEAR:
                outward(back, step, k).wait_recv()
        across(step).start()

    p_refs = (pr_ref, pi_ref, q_ref)
    widen(all_ref, wide_ref, core)
    turn(wide_ref, core, p_refs)
    onehot, rows, which = station_maps(wide_ref, core)
    for step in range(4):
        across(step).wait_recv()
    widen(all_ref, wide_ref, 1 - core)
    turn(wide_ref, 1 - core, p_refs)
    gr, gi = solve(gr, gi, onehot, rows, p_refs)
    for part_at, g in enumerate((gr, gi)):
        turned = g.T
        at = [(n % 4) * 4 + n // 4 for n in range(NB)]
        solved_ref[part_at : part_at + 1, :] = jnp.concatenate([turned[n : n + 1, :] for n in at], axis=1)

    owners_done(got_rows, 0, keep_rows)
    lines_ref[...] = got_rows[...].astype(F32).reshape(512, 128)
    residual_rows(gr, gi, which, lines_ref, got_ints, res_ref)

    def half_tile(s, half):
        at = pl.ds(pl.multiple_of((s * 2 + half) * 8, 8), 8)
        place, vvalue = doubled(vblock_ref[at, :]), vvalue_ref[at, :]
        values = [vvalue * res_ref[p, half, pl.ds(s, 1), :] for p in range(2)]
        return spread_out(place, values)

    def grid_step(step, acc):
        for piece_at in range(4):
            group = step * 4 + piece_at
            members = [half_tile(group * 8 + member, half) for member in range(8) for half in range(2)]
            left = left_ref[:, pl.ds(pl.multiple_of(group * 2048, 2048), 2048)]
            right = jnp.concatenate(members, axis=1)
            acc = acc + lax.dot_general(right, left, (((1,), (1,)), ((), ())), preferred_element_type=F32)
        return acc

    acc = lax.fori_loop(0, NT // 32, grid_step, jnp.zeros((2 * TS, TS), F32))
    grid_ref[0] = acc[:TS].T
    grid_ref[1] = acc[TS:].T

    for k in range(2):
        line(k).wait_send()
        for step in range(1, 4):
            inward(step, k).wait_send()
            for back in range(4):
                outward(back, step, k).wait_send()
    for step in range(1, 4):
        piece(step).wait_send()
    for step in range(4):
        across(step).wait_send()


def whole(*operands):
    dma, regular = pltpu.SemaphoreType.DMA, pltpu.SemaphoreType.REGULAR
    return pl.pallas_call(
        kernel,
        name="whole",
        out_shape=(
            jax.ShapeDtypeStruct((2, TS, TS), F32),
            jax.ShapeDtypeStruct((2, S), F32),
        ),
        in_specs=[SM] + [VM] * 7,
        out_specs=(VM, VM),
        scratch_shapes=[
            pltpu.VMEM((512, 256), BF16),
            pltpu.VMEM((256, 256), BF16),
            pltpu.VMEM((4, 8, 256), F32),
            pltpu.VMEM((NT, 8, 128), BF16),
            pltpu.VMEM((NT, 4, 128), I32),
            pltpu.VMEM((3, 8, 256), F32),
            pltpu.VMEM((2, 4, 4, 8, 16, 128), BF16),
            pltpu.VMEM((NT, 8, 128), BF16),
            pltpu.VMEM((NT, 4, 128), I32),
            pltpu.VMEM((4096, 128), F32),
            pltpu.VMEM((1024, 128), F32),
            pltpu.VMEM((1024, 128), F32),
            pltpu.VMEM((1024, 128), F32),
            pltpu.VMEM((512, 128), F32),
            pltpu.VMEM((2, 2, NT, 128), F32),
            pltpu.VMEM((TS, NT * 256), BF16),
            pltpu.VMEM((NT * 16, 128), F32),
            pltpu.VMEM((NT * 16, 128), F32),
            dma((3,)), dma((3,)), dma((2,)), dma((2,)), dma((2, 3)), dma((2, 3)), dma((2, 4, 3)), dma((2, 4, 3)),
            dma((4,)), dma((4,)), dma((2,)), dma((2,)), dma((2,)), regular, regular,
        ],
        compiler_params=pltpu.CompilerParams(collective_id=0, has_side_effects=True),
    )(*operands)


def shards(pair_map, visibilities, model_vis, flag_mask, gain_amp, gain_phase, row_index, cell_codes):
    grid, solved = whole(
        pair_map, visibilities, model_vis, flag_mask, row_index[0, 0], cell_codes.reshape(2, NT, 256),
        gain_amp.reshape(4, 128), gain_phase.reshape(4, 128),
    )
    return grid[None, None], solved


def solution(mesh):
    split = Mesh(mesh.devices.reshape(2, 4, 8, 2, 2), BLK + CHAN)
    placed = (
        P(BLK, None),
        P(None, BLK, CHAN, None),
        P(None, BLK, CHAN, None),
        P(BLK, CHAN, None),
        P(),
        P(),
        P(CHAN, BLK, None, None),
        P(None, CHAN, BLK, None, None),
    )
    return jax.shard_map(
        shards,
        mesh=split,
        in_specs=placed,
        out_specs=(P(CHAN, BLK, None, None, None), P()),
        check_vma=False,
    )
```
